256 devices in a mesh: section: 4 (over y), dp: 16 (over z, core), expert: 4 (over x).
Axes of the slice: x: 4, y: 4, z: 8, core: 2. Of those that a mesh axis runs over, the one named last changes fastest.
Arguments:
- inputs: bfloat16 [4, 8192, 2048], P('section', ('dp', 'expert')), may hold values from -6 to 6
- in_cache: bfloat16 [4, 8192, 2048], P('section', ('dp', 'expert')), may hold values from -6 to 6
- out_cache: bfloat16 [4, 8192, 2048], P('section', ('dp', 'expert')), may hold values from -6 to 6
- w_up: bfloat16 [4, 2048, 57344], P('section', None, ('dp', 'expert')), may hold values from -0.125 to 0.125
- w_down: bfloat16 [4, 57344, 2048], P('section', ('dp', 'expert')), may hold values from -0.0625 to 0.0625
- routing: int32 [4, 8192, 2], P('section', ('dp', 'expert')), may hold values from 0 to 7, all different within a row; in each aligned block of 128 rows (0 to 127, 128 to 255, ..., all dimensions but the last counted through in order) at most 32 rows name the same one
- gate_table: int32 [4, 8192, 2], P('section', ('dp', 'expert')), may hold values from 1 to 16
- lengths: int32 [512], P(('dp', 'expert')), may hold values from 1 to 16
- sample_map: int32 [512], replicated, may hold values from 0 to 511, as said below
Outputs:
- next_input: bfloat16 [4, 8192, 2048], P('section', ('dp', 'expert'))
- new_out_cache: bfloat16 [4, 8192, 2048], P('section', ('dp', 'expert'))
The draws below stay inside these ranges and needn't reach their ends.
Inputs may be any that keep to these rules, and one draw needn't show every extreme that they name: `sample_map`: A permutation. Every sample keeps its index along expert; the samples of one device go to exactly 8 replicas, exactly 1 to each. `routing`: A row names 2 different experts; in the rows of one device each expert is named exactly 32 times.
All inputs are finite; a program needn't handle non-finite values.
Results may differ from the reference program's by a relative error of at most 0.007.
Values may be sent and summed in bfloat16 or wider, within the bound.
No kernel may reach another device: no remote copies, remote signals or barrier semaphores. Data moves between devices by JAX's collectives and lax.ppermute only.
A program may use at most 128 MiB of HBM per device.

```python
import math
import jax
import jax.numpy as jnp
import numpy as np
from jax import lax

D = 2048
FF = 7168
EXPERTS = 8
TOPK = 2
ROWS = 16
SAMP_DEV = 8
TOK_DEV = 128
SAMPLES = 512
TOKENS = 8192
CAP_E = 32
CAP_S = 1
N_SECTION = 4
N_DP = 16
N_EXPERT = 4


def shuffled_rows(row_key, count, length):
    return jax.vmap(lambda single_key: jax.random.permutation(single_key, length))(jax.random.split(row_key, count))


def draw_sample_map(key, part):
    block_count = SAMP_DEV // CAP_S
    columns = []
    for column in range(N_EXPERT):
        column_key = jax.random.fold_in(key, 101 + column)
        outer_perm = jax.random.permutation(jax.random.fold_in(column_key, 1), N_DP)
        inner_perm = jax.random.permutation(jax.random.fold_in(column_key, 2), N_DP)
        offsets = jax.random.permutation(jax.random.fold_in(column_key, 3), N_DP)[:block_count]
        turned = shuffled_rows(jax.random.fold_in(column_key, 4), N_DP, SAMP_DEV)
        settle = shuffled_rows(jax.random.fold_in(column_key, 5), N_DP, SAMP_DEV)
        block_ids = turned // CAP_S
        within = turned % CAP_S
        dest_rep = outer_perm[(inner_perm[:, None] + offsets[block_ids]) % N_DP]
        new_local = settle[dest_rep, block_ids * CAP_S + within]
        columns.append((dest_rep * N_EXPERT + column) * SAMP_DEV + new_local)
    stacked = jnp.stack(columns, axis=1)
    return stacked.reshape(SAMPLES).astype(jnp.int32)


def plant(array, stream_key, smallest, largest):
    shape = array.shape
    index_at = [jax.random.randint(jax.random.fold_in(stream_key, axis), (), 0, shape[axis]) for axis in range(len(shape))]
    array = array.at[tuple(index_at)].set(smallest)
    longest = shape.index(max(shape))
    index_at[longest] = (index_at[longest] + 1) % shape[longest]
    return array.at[tuple(index_at)].set(largest)


def block_levels(key, dims, cuts, low, top_value):
    factor_of = 1.0
    for dim, shards_of in cuts:
        draws = jax.random.uniform(jax.random.fold_in(jax.random.fold_in(key, 6), dim), (shards_of,), jnp.float32, low / len(cuts), top_value / len(cuts))
        factor_of = factor_of * jnp.repeat(jnp.exp(draws), dims[dim] // shards_of).reshape((-1,) + (1,) * (len(dims) - 1 - dim))
    return factor_of


def routed_block(own_key, own, number, rows, count, top, most, slope):
    sequence = jax.random.permutation(own_key, count)
    heavy_load, ordinary = shares(count, rows * top, most, slope, True), shares(count, rows * top, most, slope, False)
    places = jnp.arange(count)

    def named(sizes, offset_by):
        used = int((sizes > 0).sum())
        fixed = max(1, used // 4)
        passed = fixed + (places - fixed + offset_by * (used - fixed)) % max(1, count - fixed)
        return jnp.zeros((count,), jnp.int32).at[sequence[jnp.where(places < fixed, places, passed)]].set(jnp.asarray(sizes, jnp.int32))

    sizes = jnp.where(number % 4 == 0, named(heavy_load, number // 4), named(ordinary, number - number // 4 - 1))
    mixed = jax.random.permutation(jax.random.fold_in(own, 3), count)
    donor, sink = mixed[0:count // 2 * 2:2], mixed[1:count // 2 * 2:2]
    slack = jnp.minimum(sizes[donor] - 1, most - sizes[sink]) // 2
    slack = jnp.where((donor == sequence[0]) | (sink == sequence[0]) | (sizes[sink] == 0), 0, jnp.maximum(slack, 0))
    passed = jax.random.randint(jax.random.fold_in(own, 4), (count // 2,), 0, 1 << 20) % (slack + 1)
    sizes = sizes.at[donor].add(-passed).at[sink].add(passed)
    items = jnp.searchsorted(jnp.cumsum(sizes), jnp.arange(rows * top), side="right").astype(jnp.int32)
    listing = items.reshape(top, rows).T
    listing = listing[jax.random.permutation(jax.random.fold_in(own, 1), rows)]
    offset_by = jax.random.randint(jax.random.fold_in(own, 2), (rows, 1), 0, top)
    return jnp.take_along_axis(listing, (jnp.arange(top)[None, :] + offset_by) % top, axis=1)


def shares(number_of, total, most, skew, full):
    loads = [(1 << 20) // math.isqrt(grade ** skew) + 1 for grade in range(1, number_of + 1)]
    largest = most if full else min(most, max(-(-total // number_of), total * loads[0] // sum(loads)))
    least = 1 if total - largest >= number_of - 1 else 0
    holding, surplus = [largest] + [least] * (number_of - 1), total - largest - least * (number_of - 1)
    while surplus > 0:
        free = [i for i in range(1, number_of) if holding[i] < largest] or [i for i in range(1, number_of) if holding[i] < most]
        mass, remaining = sum([loads[i] for i in free]), surplus
        for i in free:
            more = min(most - holding[i], max(1, remaining * loads[i] // mass), surplus)
            holding[i] = holding[i] + more
            surplus = surplus - more
    return np.array(holding)


def scatter_about(own_key, dims, scale, most, cuts=(), held_as=jnp.bfloat16):
    result = scale * jax.random.normal(own_key, dims, jnp.float32)
    if cuts:
        result = result * block_levels(own_key, dims, cuts, -0.22, 0.18)
    return jnp.clip(result, -most, most).astype(held_as)


def setup_inputs(seed: int = 0) -> dict:
    key_of = jax.random.split(jax.random.key(seed), 10)
    inputs = scatter_about(key_of[0], (N_SECTION, TOKENS, D), 1.0, 6.0, ((0, 4), (1, 64)))
    in_cache = scatter_about(key_of[1], (N_SECTION, TOKENS, D), 1.0, 6.0, ((0, 4), (1, 64)))
    out_cache = scatter_about(key_of[2], (N_SECTION, TOKENS, D), 1.0, 6.0, ((0, 4), (1, 64)))
    w_up = scatter_about(key_of[3], (N_SECTION, D, EXPERTS * FF), D ** -0.5, 0.125, ((0, 4), (2, 64)))
    w_down = scatter_about(key_of[4], (N_SECTION, EXPERTS * FF, D), FF ** -0.5, 0.0625, ((0, 4), (1, 64)))
    routing_keys = jax.random.split(jax.random.fold_in(key_of[5], 1), N_SECTION * TOKENS // TOK_DEV)
    routing_turns = jax.random.permutation(jax.random.fold_in(key_of[5], 3), N_SECTION * TOKENS // TOK_DEV)
    routing = jax.vmap(lambda own, number: routed_block(jax.random.fold_in(key_of[5], 2), own, number, TOK_DEV, EXPERTS, TOPK, CAP_E, 0))(routing_keys, routing_turns).reshape((N_SECTION, TOKENS, TOPK))
    gate_table = plant(jax.random.randint(key_of[6], (N_SECTION, TOKENS, TOPK), 1, 17), jax.random.fold_in(key_of[6], 1), 1, 16).astype(jnp.int32)
    lengths = plant(jax.random.randint(key_of[7], (SAMPLES,), 1, ROWS + 1), jax.random.fold_in(key_of[7], 1), 1, ROWS).astype(jnp.int32)
    sample_map = draw_sample_map(jax.random.fold_in(key_of[9], 71), 0)
    return dict(inputs=inputs, in_cache=in_cache, out_cache=out_cache, w_up=w_up, w_down=w_down, routing=routing, gate_table=gate_table, lengths=lengths, sample_map=sample_map)


def reference(inputs, in_cache, out_cache, w_up, w_down, routing, gate_table, lengths, sample_map):
    feature_width = inputs.shape[2]
    total_samples = sample_map.shape[0]
    sources = jnp.zeros((total_samples,), jnp.int32).at[sample_map].set(jnp.arange(total_samples, dtype=jnp.int32))

    def migrate(cache):
        shaped = cache.reshape(N_SECTION, total_samples, ROWS, feature_width)
        return shaped[:, sources].reshape(N_SECTION, total_samples * ROWS, feature_width)

    in_moved = migrate(in_cache)
    out_moved = migrate(out_cache)
    slice_count = N_DP * N_EXPERT // EXPERTS
    slice_width = FF // slice_count
    per_expert = total_samples * ROWS * TOPK // EXPERTS

    def expert_layer(section_args):
        tokens, up_section, down_section, chosen, gates = section_args
        flat_experts = chosen.reshape(-1)
        sorted_order = jnp.argsort(flat_experts, stable=True).astype(jnp.int32)
        grouped = tokens[sorted_order // TOPK].reshape(EXPERTS, per_expert, feature_width)
        up_all = up_section.reshape(feature_width, EXPERTS, FF).transpose(1, 0, 2)
        down_all = down_section.reshape(EXPERTS, FF, feature_width)

        def one_expert(expert_args):
            rows_here, up_here, down_here = expert_args
            hidden = jax.nn.silu(jnp.dot(rows_here, up_here, preferred_element_type=jnp.float32)).astype(jnp.bfloat16)
            pieces = jnp.einsum("rsf,sfd->srd",
                                hidden.reshape(per_expert, slice_count, slice_width).astype(jnp.float32),
                                down_here.reshape(slice_count, slice_width, feature_width).astype(jnp.float32))
            rounded = lax.optimization_barrier(pieces.astype(jnp.bfloat16)).astype(jnp.float32)
            return jnp.sum(rounded, axis=0)

        expert_rows = lax.map(one_expert, (grouped, up_all, down_all)).reshape(-1, feature_width)
        position = jnp.zeros_like(sorted_order).at[sorted_order].set(jnp.arange(sorted_order.shape[0], dtype=jnp.int32))
        per_assign = expert_rows[position].reshape(tokens.shape[0], TOPK, feature_width)
        weights = gates.astype(jnp.float32)
        weights = weights / jnp.sum(weights, axis=1, keepdims=True)
        return jnp.sum(weights[:, :, None] * per_assign, axis=1)

    mixed = lax.map(expert_layer, (inputs, w_up, w_down, routing, gate_table))
    valid_rows = (jnp.arange(ROWS, dtype=jnp.int32)[None, :] < lengths[:, None]).reshape(-1)
    delta_rows = jnp.where(valid_rows[None, :, None], (mixed - out_moved.astype(jnp.float32)).astype(jnp.bfloat16), jnp.zeros((), jnp.bfloat16))
    new_out_cache = (out_moved.astype(jnp.float32) + delta_rows.astype(jnp.float32)).astype(jnp.bfloat16)
    received = jnp.concatenate([jnp.zeros_like(delta_rows[:1]), delta_rows[:-1]], axis=0)
    next_input = (in_moved.astype(jnp.float32) + received.astype(jnp.float32)).astype(jnp.bfloat16)
    return next_input, new_out_cache
```

```python
import functools

import jax
import jax.numpy as jnp
from jax import lax
from jax.experimental import pallas as pl
from jax.experimental.pallas import tpu as pltpu
from jax.sharding import Mesh, PartitionSpec as P

EXPERTS = 8
TOPK = 2
ROWS = 16
SAMP_DEV = 8
BF16 = jnp.bfloat16
F32 = jnp.float32


def shifted(value, axis, by):
    peers = lax.axis_size(axis)
    return lax.ppermute(value, axis, [(i, (i + by) % peers) for i in range(peers)])


def group_kernel(routing_ref, tokens_ref, grouped_ref, slot_ref):
    rows = routing_ref.shape[0]
    slots = grouped_ref.shape[0]
    per_expert = slots // EXPERTS
    routing = routing_ref[...]
    lanes = lax.broadcasted_iota(jnp.int32, (rows, rows), 1)
    earlier = (lax.broadcasted_iota(jnp.int32, (rows, rows), 0) > lanes).astype(BF16)
    first = (routing[:, 0:1] == lanes).astype(F32)
    second = (routing[:, 1:2] == lanes).astype(F32)
    before_first = jnp.dot(earlier, first.astype(BF16), preferred_element_type=F32)
    before_second = jnp.dot(earlier, second.astype(BF16), preferred_element_type=F32) + jnp.sum(
        first, axis=0, keepdims=True
    )
    base = (lanes * per_expert).astype(F32)
    slot_first = jnp.sum(first * (before_first + base), axis=1, keepdims=True).astype(jnp.int32)
    slot_second = jnp.sum(second * (before_second + base), axis=1, keepdims=True).astype(jnp.int32)
    slot_lanes = lax.broadcasted_iota(jnp.int32, (rows, slots), 1)
    chosen = ((slot_first == slot_lanes) | (slot_second == slot_lanes)).astype(F32).astype(BF16)
    grouped_ref[...] = lax.dot_general(
        chosen, tokens_ref[...], (((0,), (0,)), ((), ())), preferred_element_type=F32
    ).astype(BF16)
    slot_ref[:, 0:1] = slot_first
    slot_ref[:, 1:2] = slot_second


def group_rows(routing, tokens):
    rows, width = tokens.shape
    slots = rows * TOPK
    return pl.pallas_call(
        group_kernel,
        out_shape=(
            jax.ShapeDtypeStruct((slots, width), BF16),
            jax.ShapeDtypeStruct((rows, TOPK), jnp.int32),
        ),
        cost_estimate=pl.CostEstimate(
            flops=2 * slots * rows * width, bytes_accessed=3 * slots * width, transcendentals=0
        ),
        name="group_rows",
    )(routing, tokens)


def combine_kernel(back_ref, slot_ref, gate_ref, live_ref, moved_ref, delta_ref, cache_ref):
    rows = slot_ref.shape[0]
    slots = back_ref.shape[0]
    slot_lanes = lax.broadcasted_iota(jnp.int32, (rows, slots), 1)
    slot = slot_ref[...]
    back = back_ref[...]
    pick_first = (slot[:, 0:1] == slot_lanes).astype(F32).astype(BF16)
    pick_second = (slot[:, 1:2] == slot_lanes).astype(F32).astype(BF16)
    first = jnp.dot(pick_first, back, preferred_element_type=F32)
    second = jnp.dot(pick_second, back, preferred_element_type=F32)
    gates = gate_ref[...].astype(F32)
    total = gates[:, 0:1] + gates[:, 1:2]
    mixed = gates[:, 0:1] / total * first + gates[:, 1:2] / total * second
    moved = moved_ref[...].astype(F32)
    delta = jnp.where(live_ref[...] > 0, mixed - moved, 0.0).astype(BF16)
    delta_ref[...] = delta
    cache_ref[...] = (moved + delta.astype(F32)).astype(BF16)


def combine(back, slot, gates, live, moved):
    rows, width = moved.shape
    out = jax.ShapeDtypeStruct((rows, width), BF16)
    return pl.pallas_call(
        combine_kernel,
        out_shape=(out, out),
        cost_estimate=pl.CostEstimate(
            flops=4 * back.shape[0] * rows * width,
            bytes_accessed=2 * back.size + 6 * moved.size,
            transcendentals=0,
        ),
        name="combine",
    )(back, slot, gates, live, moved)


def per_device(
    inputs, in_cache, out_cache, w_up, w_down, routing, gate_table, lengths, sample_map
):
    width = inputs.shape[2]
    tok_rows = inputs.shape[1]
    z_count = lax.axis_size("z")
    x_count = lax.axis_size("x")
    dp_count = z_count * lax.axis_size("core")
    own_dp = lax.axis_index(("z", "core"))
    own_device = own_dp * x_count + lax.axis_index("x")

    grouped, slot = group_rows(routing[0], inputs[0])
    up_own, down_own = w_up[0], w_down[0]
    up_other = shifted(up_own, "core", 1)
    down_other = shifted(down_own, "core", 1)
    block = lax.all_to_all(
        grouped.reshape(z_count, -1, width), "z", split_axis=0, concat_axis=0, tiled=True
    ).reshape(-1, width)
    half = block.shape[0] // 2
    from_left = shifted(block, "x", 1)
    from_right = shifted(block, "x", -1)
    far_top = shifted(from_left[:half], "x", 1)
    far_bottom = shifted(from_right[half:], "x", -1)

    def expert(rows):
        hidden_own = jax.nn.silu(jnp.dot(rows, up_own, preferred_element_type=F32)).astype(BF16)
        hidden_other = jax.nn.silu(jnp.dot(rows, up_other, preferred_element_type=F32)).astype(BF16)
        return (
            jnp.dot(hidden_own, down_own, preferred_element_type=F32)
            + jnp.dot(hidden_other, down_other, preferred_element_type=F32)
        ).astype(BF16)

    out_own = expert(block)
    out_left = expert(from_left)
    out_right = expert(from_right)
    out_far_top = expert(far_top)
    out_far_bottom = expert(far_bottom)

    top = shifted(out_far_top, "x", -1)
    bottom = shifted(out_far_bottom, "x", 1)
    to_left = jnp.concatenate(
        [(out_left[:half].astype(F32) + top.astype(F32)).astype(BF16), out_left[half:]]
    )
    to_right = jnp.concatenate(
        [out_right[:half], (out_right[half:].astype(F32) + bottom.astype(F32)).astype(BF16)]
    )
    got_right = shifted(to_left, "x", -1)
    got_left = shifted(to_right, "x", 1)
    summed = (
        out_own.astype(F32) + got_right.astype(F32) + got_left.astype(F32)
    ).astype(BF16)
    back = lax.all_to_all(
        summed.reshape(z_count, -1, width), "z", split_axis=0, concat_axis=0, tiled=True
    ).reshape(-1, width)

    own_map = lax.dynamic_slice_in_dim(sample_map, own_device * SAMP_DEV, SAMP_DEV)
    dest_dp = own_map // SAMP_DEV // x_count
    sample_ids = jnp.arange(SAMP_DEV, dtype=jnp.int32)
    goes = dest_dp[None, :] == jnp.arange(dp_count, dtype=jnp.int32)[:, None]
    slot_sample = jnp.sum(jnp.where(goes, sample_ids[None, :], 0), axis=1)
    own_places = own_device * SAMP_DEV + sample_ids
    sources = jnp.sum(
        jnp.where(
            sample_map[None, :] == own_places[:, None],
            jnp.arange(sample_map.shape[0], dtype=jnp.int32)[None, :],
            0,
        ),
        axis=1,
    )
    source_dp = sources // SAMP_DEV // x_count

    def migrate(cache):
        sent = cache.reshape(SAMP_DEV, ROWS, width)[slot_sample]
        got = lax.all_to_all(sent, ("z", "core"), split_axis=0, concat_axis=0, tiled=True)
        return got[source_dp].reshape(tok_rows, width)

    out_moved = migrate(out_cache[0])
    in_moved = migrate(in_cache[0])

    live = (
        jnp.arange(tok_rows, dtype=jnp.int32) % ROWS < jnp.repeat(lengths, ROWS)
    ).astype(jnp.int32)[:, None]
    delta, new_out = combine(back, slot, gate_table[0], live, out_moved)
    sections = lax.axis_size("section")
    received = lax.ppermute(delta, "section", [(i, i + 1) for i in range(sections - 1)])
    next_input = (in_moved.astype(F32) + received.astype(F32)).astype(BF16)
    return next_input[None], new_out[None]


def solution(mesh):
    sections, dp, expert = mesh.devices.shape
    split = Mesh(
        mesh.devices.reshape(sections, dp // 2, 2, expert), ("section", "z", "core", "x")
    )
    group = ("z", "core", "x")
    rows = P("section", group, None)
    placed = (rows, rows, rows, P("section", None, group), rows, rows, rows, P(group), P())
    return jax.shard_map(
        per_device, mesh=split, in_specs=placed, out_specs=(rows, rows), check_vma=False
    )
```

```python
import functools

import jax
import jax.numpy as jnp
from jax import lax
from jax.experimental import pallas as pl
from jax.experimental.pallas import tpu as pltpu
from jax.sharding import Mesh, PartitionSpec as P

EXPERTS = 8
TOPK = 2
ROWS = 16
SAMP_DEV = 8
ROW_CHUNKS = 2
FEATURE_CHUNKS = 2
UP_STEP = 512
DOWN_STEP = 512
BF16 = jnp.bfloat16
F32 = jnp.float32


def shifted(value, axis, by):
    peers = lax.axis_size(axis)
    return lax.ppermute(value, axis, [(i, (i + by) % peers) for i in range(peers)])


def join_kernel(*refs):
    at = 0
    for ref in refs[:-1]:
        refs[-1][at : at + ref.shape[0]] = ref[...]
        at += ref.shape[0]


def join(pieces):
    rows = sum(piece.shape[0] for piece in pieces)
    return pl.pallas_call(
        join_kernel,
        out_shape=jax.ShapeDtypeStruct((rows, pieces[0].shape[1]), BF16),
        cost_estimate=pl.CostEstimate(
            flops=1000000, bytes_accessed=4 * rows * pieces[0].shape[1], transcendentals=0
        ),
    )(*pieces)


def group_kernel(plane_ref, routing_ref, tokens_ref, *out_refs):
    piece_refs, slot_ref = out_refs[:-1], out_refs[-1]
    rows = tokens_ref.shape[0]
    per_expert = rows * TOPK // EXPERTS
    part = per_expert // ROW_CHUNKS
    experts = lax.broadcasted_iota(jnp.int32, (2 * EXPERTS, rows), 0)
    earlier = (
        lax.broadcasted_iota(jnp.int32, (rows, rows), 0)
        < lax.broadcasted_iota(jnp.int32, (rows, rows), 1)
    ).astype(F32).astype(BF16)
    routing = (routing_ref[...] + (EXPERTS - plane_ref[0])) % EXPERTS
    first = (routing[0:1, :] == experts).astype(F32)
    second = (routing[1:2, :] == experts).astype(F32)
    before_first = jnp.dot(first.astype(BF16), earlier, preferred_element_type=F32)
    before_second = jnp.dot(second.astype(BF16), earlier, preferred_element_type=F32) + jnp.sum(
        first, axis=1, keepdims=True
    )
    base = (experts * per_expert).astype(F32)
    slot_first = jnp.sum(first * (before_first + base), axis=0, keepdims=True).astype(jnp.int32)
    slot_second = jnp.sum(second * (before_second + base), axis=0, keepdims=True).astype(jnp.int32)
    slot_ref[0:1, :] = slot_first
    slot_ref[1:2, :] = slot_second
    tokens = tokens_ref[...]
    index = lax.broadcasted_iota(jnp.int32, (EXPERTS * part, rows), 0)
    for chunk in range(ROW_CHUNKS):
        wanted = index // part * per_expert + chunk * part + index % part
        chosen = ((slot_first == wanted) | (slot_second == wanted)).astype(F32).astype(BF16)
        picked = jnp.dot(chosen, tokens, preferred_element_type=F32).astype(BF16)
        for expert in range(EXPERTS):
            piece_refs[chunk * EXPERTS + expert][...] = picked[expert * part : (expert + 1) * part]


def group_rows(plane, routing, tokens):
    rows, width = tokens.shape
    slots = rows * TOPK
    pieces = ROW_CHUNKS * EXPERTS
    piece = jax.ShapeDtypeStruct((slots // pieces, width), BF16)
    vmem = pl.BlockSpec(memory_space=pltpu.VMEM)
    out = pl.pallas_call(
        group_kernel,
        in_specs=[pl.BlockSpec(memory_space=pltpu.SMEM), vmem, vmem],
        out_shape=(piece,) * pieces + (jax.ShapeDtypeStruct((TOPK, rows), jnp.int32),),
        cost_estimate=pl.CostEstimate(
            flops=2 * slots * rows * width, bytes_accessed=3 * slots * width, transcendentals=0
        ),
        name="group_rows",
    )(plane, routing, tokens)
    return [out[c * EXPERTS : (c + 1) * EXPERTS] for c in range(ROW_CHUNKS)], out[-1]


def up_kernel(count, *refs):
    row_refs, own_ref, other_ref = refs[:count], refs[count], refs[count + 1]
    out_refs, total_ref = refs[count + 2 : -1], refs[-1]
    step = pl.program_id(0)
    rows = jnp.concatenate([ref[...] for ref in row_refs], axis=0)
    weights = jnp.concatenate([own_ref[...], other_ref[...]], axis=1)
    term = jnp.dot(rows, weights, preferred_element_type=F32)

    @pl.when(step == 0)
    def _():
        total_ref[...] = term

    @pl.when((step > 0) & (step < pl.num_programs(0) - 1))
    def _():
        total_ref[...] += term

    @pl.when(step == pl.num_programs(0) - 1)
    def _():
        value = total_ref[...] + term
        hidden = (value / (1.0 + jnp.exp(-value))).astype(BF16)
        at = 0
        for ref in out_refs:
            ref[...] = hidden[at : at + ref.shape[0]]
            at += ref.shape[0]


def up(blocks, own, other):
    depth, units = own.shape
    count = len(blocks)
    total = sum(block.shape[0] for block in blocks)
    weight = pl.BlockSpec((UP_STEP, units), lambda k: (k, 0))
    return pl.pallas_call(
        functools.partial(up_kernel, count),
        grid=(depth // UP_STEP,),
        in_specs=[pl.BlockSpec((block.shape[0], UP_STEP), lambda k: (0, k)) for block in blocks]
        + [weight, weight],
        out_specs=[pl.BlockSpec((block.shape[0], 2 * units), lambda k: (0, 0)) for block in blocks],
        out_shape=[jax.ShapeDtypeStruct((block.shape[0], 2 * units), BF16) for block in blocks],
        scratch_shapes=[pltpu.VMEM((total, 2 * units), F32)],
        cost_estimate=pl.CostEstimate(
            flops=4 * total * depth * units,
            bytes_accessed=4 * depth * units + 2 * total * depth,
            transcendentals=2 * total * units,
        ),
    )(*blocks, own, other)


def down_kernel(count, added, split, *refs):
    hidden_refs, own_ref, other_ref = refs[:count], refs[count], refs[count + 1]
    outs = split or len(added)
    extra_refs = refs[count + 2 : len(refs) - outs]
    out_refs = refs[len(refs) - outs :]
    piece_refs = out_refs
    hidden = jnp.concatenate([ref[...] for ref in hidden_refs], axis=0)
    weights = jnp.concatenate([own_ref[...], other_ref[...]], axis=0)
    term = jnp.dot(hidden, weights, preferred_element_type=F32)
    rows = hidden_refs[0].shape[0]
    at = 0
    for parts, out_ref in zip(added, out_refs):
        for number, operands in enumerate(parts):
            value = term[at : at + rows]
            for which, lead in operands:
                extra = extra_refs[which]
                value += (extra[...] if lead is None else extra[lead]).astype(F32)
            value = value.astype(BF16)
            if split:
                part = rows // split
                for piece in range(split):
                    piece_refs[piece][number * part : (number + 1) * part] = value[
                        piece * part : (piece + 1) * part
                    ]
            elif len(parts) == 1:
                out_ref[...] = value
            else:
                out_ref[number] = value
            at += rows


def down(hidden, own, other, chunk, added, extras=(), split=0):
    rows, units = hidden[0].shape
    units //= 2
    width = own.shape[1] // FEATURE_CHUNKS
    steps = width // DOWN_STEP
    weight = pl.BlockSpec((units, DOWN_STEP), lambda n: (0, chunk * steps + n))
    out_shape, out_specs = [], []
    for parts in added:
        if split:
            lead = (len(parts) * rows // split,)
        elif len(parts) == 1:
            lead = (rows,)
        else:
            lead = (len(parts), rows)
        out_shape.append(jax.ShapeDtypeStruct(lead + (width,), BF16))
        out_specs.append(
            pl.BlockSpec(lead + (DOWN_STEP,), lambda n, lead=lead: (0,) * len(lead) + (n,))
        )
    out_shape, out_specs = out_shape * max(1, split), out_specs * max(1, split)
    total = rows * len(hidden)
    return pl.pallas_call(
        functools.partial(down_kernel, len(hidden), added, split),
        grid=(steps,),
        in_specs=[pl.BlockSpec((rows, 2 * units), lambda n: (0, 0)) for _ in hidden]
        + [weight, weight]
        + [
            pl.BlockSpec(
                extra.shape[:-1] + (DOWN_STEP,), lambda n, rank=extra.ndim: (0,) * (rank - 1) + (n,)
            )
            for extra in extras
        ],
        out_specs=out_specs,
        out_shape=out_shape,
        cost_estimate=pl.CostEstimate(
            flops=4 * total * width * units,
            bytes_accessed=4 * width * units + 2 * total * width,
            transcendentals=0,
        ),
    )(*hidden, own, other, *extras)


def combine_kernel(slot_ref, gate_ref, live_ref, moved_ref, *refs):
    back_refs, (delta_ref, cache_ref) = refs[:-2], refs[-2:]
    rows = slot_ref.shape[0]
    back = jnp.concatenate([ref[...] for ref in back_refs], axis=0)
    slots = back.shape[0]
    slot_lanes = lax.broadcasted_iota(jnp.int32, (rows, slots), 1)
    slot = slot_ref[...]
    pick_first = (slot[:, 0:1] == slot_lanes).astype(F32).astype(BF16)
    pick_second = (slot[:, 1:2] == slot_lanes).astype(F32).astype(BF16)
    first = jnp.dot(pick_first, back, preferred_element_type=F32)
    second = jnp.dot(pick_second, back, preferred_element_type=F32)
    gates = gate_ref[...].astype(F32)
    total = gates[:, 0:1] + gates[:, 1:2]
    mixed = gates[:, 0:1] / total * first + gates[:, 1:2] / total * second
    moved = moved_ref[...].astype(F32)
    delta = jnp.where(live_ref[...] > 0, mixed - moved, 0.0).astype(BF16)
    delta_ref[...] = delta
    cache_ref[...] = (moved + delta.astype(F32)).astype(BF16)


def combine(back, slot, gates, live, moved):
    rows, width = moved.shape
    out = jax.ShapeDtypeStruct((rows, width), BF16)
    return pl.pallas_call(
        combine_kernel,
        out_shape=(out, out),
        cost_estimate=pl.CostEstimate(
            flops=4 * TOPK * rows * rows * width,
            bytes_accessed=(2 * TOPK + 6) * moved.size,
            transcendentals=0,
        ),
    )(slot, gates, live, moved, *back)


def section_step(
    inputs, in_cache, out_cache, w_up, w_down, routing, gate_table, lengths, sample_map
):
    width = inputs.shape[2]
    tok_rows = inputs.shape[1]
    z_count = lax.axis_size("z")
    x_count = lax.axis_size("x")
    dp_count = z_count * lax.axis_size("core")
    own_dp = lax.axis_index(("z", "core"))
    own_device = own_dp * x_count + lax.axis_index("x")

    plane = lax.axis_index("z").astype(jnp.int32)[None]
    chunks, slot = group_rows(plane, routing[0].T, inputs[0])
    up_own, down_own = w_up[0], w_down[0]
    order = sorted(range(1, z_count), key=lambda away: -min(away, z_count - away))
    blocks = []
    for pieces in chunks:
        got = {away: shifted(pieces[away], "z", away) for away in order}
        blocks.append(join([pieces[0]] + [got[away] for away in range(1, z_count)]))
    up_other = shifted(up_own, "core", 1)
    down_other = shifted(down_own, "core", 1)
    from_left = [shifted(block, "x", 1) for block in blocks]
    from_right = [shifted(block, "x", -1) for block in blocks]
    far = [shifted(from_left[0], "x", 1), shifted(from_right[1], "x", -1)]
    near_hidden = [
        up([blocks[c], from_left[c], from_right[c]], up_own, up_other)
        for c in range(ROW_CHUNKS)
    ]
    far_hidden = [up([far[c]], up_own, up_other)[0] for c in range(ROW_CHUNKS)]
    own_hidden = [hidden[0] for hidden in near_hidden]
    side_hidden = [hidden[1] for hidden in near_hidden] + [hidden[2] for hidden in near_hidden]

    backs = []
    for f in range(FEATURE_CHUNKS):
        far_first, far_second = down(far_hidden, down_own, down_other, f, (((),), ((),)))
        for_left = shifted(far_first, "x", -1)
        for_right = shifted(far_second, "x", 1)
        to_left, to_right = down(
            side_hidden,
            down_own,
            down_other,
            f,
            ((((0, None),), ()), ((), ((1, None),))),
            (for_left, for_right),
        )
        got_right = shifted(to_left, "x", -1)
        got_left = shifted(to_right, "x", 1)
        summed = down(
            own_hidden,
            down_own,
            down_other,
            f,
            ((((0, 0), (1, 0)), ((0, 1), (1, 1))),),
            (got_left, got_right),
            split=z_count,
        )
        got = {away: shifted(summed[away], "z", -away) for away in order}
        backs.append([summed[0]] + [got[away] for away in range(1, z_count)])

    own_map = lax.dynamic_slice_in_dim(sample_map, own_device * SAMP_DEV, SAMP_DEV)
    dest_dp = own_map // SAMP_DEV // x_count
    sample_ids = jnp.arange(SAMP_DEV, dtype=jnp.int32)
    goes = dest_dp[None, :] == jnp.arange(dp_count, dtype=jnp.int32)[:, None]
    slot_sample = jnp.sum(jnp.where(goes, sample_ids[None, :], 0), axis=1)
    own_places = own_device * SAMP_DEV + sample_ids
    sources = jnp.sum(
        jnp.where(
            sample_map[None, :] == own_places[:, None],
            jnp.arange(sample_map.shape[0], dtype=jnp.int32)[None, :],
            0,
        ),
        axis=1,
    )
    source_dp = sources // SAMP_DEV // x_count

    slot_sample, _ = lax.optimization_barrier((slot_sample, blocks[1]))
    sent = jnp.concatenate(
        [
            cache.reshape(SAMP_DEV, 1, ROWS, width)[slot_sample]
            for cache in (out_cache[0], in_cache[0])
        ],
        axis=1,
    )
    got = lax.all_to_all(sent, ("z", "core"), split_axis=0, concat_axis=0, tiled=True)
    moved = got[source_dp]
    out_moved = moved[:, 0].reshape(tok_rows, width)
    in_moved = moved[:, 1].reshape(tok_rows, width)

    live = (
        jnp.arange(tok_rows, dtype=jnp.int32) % ROWS < jnp.repeat(lengths, ROWS)
    ).astype(jnp.int32)[:, None]
    slot = slot.T
    sections = lax.axis_size("section")
    caches, arrivals = [], []
    part = width // FEATURE_CHUNKS
    for f, back in enumerate(backs):
        columns = out_moved[:, f * part : (f + 1) * part]
        delta, cache = combine(back, slot, gate_table[0], live, columns)
        caches.append(cache)
        arrivals.append(lax.ppermute(delta, "section", [(i, i + 1) for i in range(sections - 1)]))
    new_out = jnp.concatenate(caches, axis=1)
    received = jnp.concatenate(arrivals, axis=1)
    next_input = (in_moved.astype(F32) + received.astype(F32)).astype(BF16)
    return next_input[None], new_out[None]


def solution(mesh):
    sections, dp, expert = mesh.devices.shape
    split = Mesh(
        mesh.devices.reshape(sections, dp // 2, 2, expert), ("section", "z", "core", "x")
    )
    group = ("z", "core", "x")
    rows = P("section", group, None)
    placed = (rows, rows, rows, P("section", None, group), rows, rows, rows, P(group), P())
    return jax.shard_map(
        section_step, mesh=split, in_specs=placed, out_specs=(rows, rows), check_vma=False
    )
```

```python
import functools

import jax
import jax.numpy as jnp
from jax import lax
from jax.experimental import pallas as pl
from jax.experimental.pallas import tpu as pltpu
from jax.sharding import Mesh, PartitionSpec as P

EXPERTS = 8
TOPK = 2
ROWS = 16
SAMP_DEV = 8
ROW_CHUNKS = 2
FEATURE_CHUNKS = 2
UP_STEP = 512
DOWN_STEP = 512
SMALL_VMEM = 8 << 20
LARGE_VMEM = 28 << 20
BF16 = jnp.bfloat16
F32 = jnp.float32


def shifted(value, axis, by):
    peers = lax.axis_size(axis)
    return lax.ppermute(value, axis, [(i, (i + by) % peers) for i in range(peers)])


def exchanged(value):
    return lax.all_to_all(value, "z", split_axis=0, concat_axis=0, tiled=True)


def group_kernel(routing_ref, tokens_ref, *out_refs):
    chunk_refs, slot_ref = out_refs[:-1], out_refs[-1]
    rows = tokens_ref.shape[0]
    per_expert = rows * TOPK // EXPERTS
    part = per_expert // ROW_CHUNKS
    experts = lax.broadcasted_iota(jnp.int32, (2 * EXPERTS, rows), 0)
    earlier = (
        lax.broadcasted_iota(jnp.int32, (rows, rows), 0)
        < lax.broadcasted_iota(jnp.int32, (rows, rows), 1)
    ).astype(F32).astype(BF16)
    first = (routing_ref[0:1, :] == experts).astype(F32)
    second = (routing_ref[1:2, :] == experts).astype(F32)
    before_first = jnp.dot(first.astype(BF16), earlier, preferred_element_type=F32)
    before_second = jnp.dot(second.astype(BF16), earlier, preferred_element_type=F32) + jnp.sum(
        first, axis=1, keepdims=True
    )
    base = (experts * per_expert).astype(F32)
    slot_first = jnp.sum(first * (before_first + base), axis=0, keepdims=True).astype(jnp.int32)
    slot_second = jnp.sum(second * (before_second + base), axis=0, keepdims=True).astype(jnp.int32)
    slot_ref[0:1, :] = slot_first
    slot_ref[1:2, :] = slot_second
    tokens = tokens_ref[...]
    index = lax.broadcasted_iota(jnp.int32, (EXPERTS * part, rows), 0)
    for chunk, chunk_ref in enumerate(chunk_refs):
        wanted = index // part * per_expert + chunk * part + index % part
        chosen = ((slot_first == wanted) | (slot_second == wanted)).astype(F32).astype(BF16)
        chunk_ref[...] = jnp.dot(chosen, tokens, preferred_element_type=F32).astype(BF16)


def group_rows(routing, tokens):
    rows, width = tokens.shape
    slots = rows * TOPK
    chunk = jax.ShapeDtypeStruct((slots // ROW_CHUNKS, width), BF16)
    out = pl.pallas_call(
        group_kernel,
        out_shape=(chunk,) * ROW_CHUNKS + (jax.ShapeDtypeStruct((TOPK, rows), jnp.int32),),
        compiler_params=pltpu.CompilerParams(vmem_limit_bytes=SMALL_VMEM),
        cost_estimate=pl.CostEstimate(
            flops=2 * slots * rows * width, bytes_accessed=3 * slots * width, transcendentals=0
        ),
        name="group_rows",
    )(routing, tokens)
    return out[:-1], out[-1]


def up_kernel(count, *refs):
    row_refs, own_ref, other_ref = refs[:count], refs[count], refs[count + 1]
    out_refs, total_ref = refs[count + 2 : -1], refs[-1]
    step = pl.program_id(0)
    rows = jnp.concatenate([ref[...] for ref in row_refs], axis=0)
    weights = jnp.concatenate([own_ref[...], other_ref[...]], axis=1)
    term = jnp.dot(rows, weights, preferred_element_type=F32)

    @pl.when(step == 0)
    def _():
        total_ref[...] = term

    @pl.when((step > 0) & (step < pl.num_programs(0) - 1))
    def _():
        total_ref[...] += term

    @pl.when(step == pl.num_programs(0) - 1)
    def _():
        value = total_ref[...] + term
        hidden = (value / (1.0 + jnp.exp(-value))).astype(BF16)
        at = 0
        for ref in out_refs:
            ref[...] = hidden[at : at + ref.shape[0]]
            at += ref.shape[0]


def up(blocks, own, other):
    depth, units = own.shape
    count = len(blocks)
    total = sum(block.shape[0] for block in blocks)
    weight = pl.BlockSpec((UP_STEP, units), lambda k: (k, 0))
    return pl.pallas_call(
        functools.partial(up_kernel, count),
        grid=(depth // UP_STEP,),
        in_specs=[pl.BlockSpec((block.shape[0], UP_STEP), lambda k: (0, k)) for block in blocks]
        + [weight, weight],
        out_specs=[pl.BlockSpec((block.shape[0], 2 * units), lambda k: (0, 0)) for block in blocks],
        out_shape=[jax.ShapeDtypeStruct((block.shape[0], 2 * units), BF16) for block in blocks],
        scratch_shapes=[pltpu.VMEM((total, 2 * units), F32)],
        compiler_params=pltpu.CompilerParams(vmem_limit_bytes=LARGE_VMEM),
        cost_estimate=pl.CostEstimate(
            flops=4 * total * depth * units,
            bytes_accessed=4 * depth * units + 2 * total * depth,
            transcendentals=2 * total * units,
        ),
    )(*blocks, own, other)


def down_kernel(count, added, split, *refs):
    hidden_refs, own_ref, other_ref = refs[:count], refs[count], refs[count + 1]
    extra_refs = refs[count + 2 : len(refs) - len(added)]
    out_refs = refs[len(refs) - len(added) :]
    hidden = jnp.concatenate([ref[...] for ref in hidden_refs], axis=0)
    weights = jnp.concatenate([own_ref[...], other_ref[...]], axis=0)
    term = jnp.dot(hidden, weights, preferred_element_type=F32)
    rows = hidden_refs[0].shape[0]
    at = 0
    for parts, out_ref in zip(added, out_refs):
        for number, operands in enumerate(parts):
            value = term[at : at + rows]
            for which, lead in operands:
                extra = extra_refs[which]
                value += (extra[...] if lead is None else extra[lead]).astype(F32)
            value = value.astype(BF16)
            if split:
                out_ref[:, number] = value.reshape(out_ref.shape[0], *out_ref.shape[2:])
            elif len(parts) == 1:
                out_ref[...] = value
            else:
                out_ref[number] = value
            at += rows


def down(hidden, own, other, chunk, added, extras=(), split=0):
    rows, units = hidden[0].shape
    units //= 2
    width = own.shape[1] // FEATURE_CHUNKS
    steps = width // DOWN_STEP
    weight = pl.BlockSpec((units, DOWN_STEP), lambda n: (0, chunk * steps + n))
    out_shape, out_specs = [], []
    for parts in added:
        if split:
            lead = (split, len(parts), rows // split)
        elif len(parts) == 1:
            lead = (rows,)
        else:
            lead = (len(parts), rows)
        out_shape.append(jax.ShapeDtypeStruct(lead + (width,), BF16))
        out_specs.append(
            pl.BlockSpec(lead + (DOWN_STEP,), lambda n, lead=lead: (0,) * len(lead) + (n,))
        )
    total = rows * len(hidden)
    return pl.pallas_call(
        functools.partial(down_kernel, len(hidden), added, split),
        grid=(steps,),
        in_specs=[pl.BlockSpec((rows, 2 * units), lambda n: (0, 0)) for _ in hidden]
        + [weight, weight]
        + [
            pl.BlockSpec(
                extra.shape[:-1] + (DOWN_STEP,), lambda n, rank=extra.ndim: (0,) * (rank - 1) + (n,)
            )
            for extra in extras
        ],
        out_specs=out_specs,
        out_shape=out_shape,
        compiler_params=pltpu.CompilerParams(vmem_limit_bytes=LARGE_VMEM),
        cost_estimate=pl.CostEstimate(
            flops=4 * total * width * units,
            bytes_accessed=4 * width * units + 2 * total * width,
            transcendentals=0,
        ),
    )(*hidden, own, other, *extras)


def combine_kernel(slot_ref, gate_ref, live_ref, moved_ref, back_ref, delta_ref, cache_ref):
    rows = slot_ref.shape[0]
    back = back_ref[...]
    slots = back.shape[0]
    slot_lanes = lax.broadcasted_iota(jnp.int32, (rows, slots), 1)
    slot = slot_ref[...]
    pick_first = (slot[:, 0:1] == slot_lanes).astype(F32).astype(BF16)
    pick_second = (slot[:, 1:2] == slot_lanes).astype(F32).astype(BF16)
    first = jnp.dot(pick_first, back, preferred_element_type=F32)
    second = jnp.dot(pick_second, back, preferred_element_type=F32)
    gates = gate_ref[...].astype(F32)
    total = gates[:, 0:1] + gates[:, 1:2]
    mixed = gates[:, 0:1] / total * first + gates[:, 1:2] / total * second
    moved = moved_ref[...].astype(F32)
    delta = jnp.where(live_ref[...] > 0, mixed - moved, 0.0).astype(BF16)
    delta_ref[...] = delta
    cache_ref[...] = (moved + delta.astype(F32)).astype(BF16)


def combine(back, slot, gates, live, moved):
    rows, width = moved.shape
    out = jax.ShapeDtypeStruct((rows, width), BF16)
    return pl.pallas_call(
        combine_kernel,
        out_shape=(out, out),
        compiler_params=pltpu.CompilerParams(vmem_limit_bytes=SMALL_VMEM),
        cost_estimate=pl.CostEstimate(
            flops=4 * TOPK * rows * rows * width,
            bytes_accessed=(2 * TOPK + 6) * moved.size,
            transcendentals=0,
        ),
    )(slot, gates, live, moved, back)


def section_step(
    inputs, in_cache, out_cache, w_up, w_down, routing, gate_table, lengths, sample_map
):
    width = inputs.shape[2]
    tok_rows = inputs.shape[1]
    z_count = lax.axis_size("z")
    x_count = lax.axis_size("x")
    dp_count = z_count * lax.axis_size("core")
    own_dp = lax.axis_index(("z", "core"))
    own_device = own_dp * x_count + lax.axis_index("x")

    chunks, slot = group_rows(routing[0].T, inputs[0])
    up_own, down_own = w_up[0], w_down[0]
    blocks = [exchanged(chunk.reshape(z_count, -1, width)).reshape(-1, width) for chunk in chunks]
    up_other = shifted(up_own, "core", 1)
    down_other = shifted(down_own, "core", 1)
    from_left = [shifted(block, "x", 1) for block in blocks]
    from_right = [shifted(block, "x", -1) for block in blocks]
    far = [shifted(from_left[0], "x", 1), shifted(from_right[1], "x", -1)]
    near_hidden = [
        up([blocks[c], from_left[c], from_right[c]], up_own, up_other)
        for c in range(ROW_CHUNKS)
    ]
    far_hidden = up(far, up_own, up_other)
    own_hidden = [hidden[0] for hidden in near_hidden]
    side_hidden = [hidden[1] for hidden in near_hidden] + [hidden[2] for hidden in near_hidden]

    backs = []
    for f in range(FEATURE_CHUNKS):
        far_first, far_second = down(far_hidden, down_own, down_other, f, (((),), ((),)))
        for_left = shifted(far_first, "x", -1)
        for_right = shifted(far_second, "x", 1)
        to_left, to_right = down(
            side_hidden,
            down_own,
            down_other,
            f,
            ((((0, None),), ()), ((), ((1, None),))),
            (for_left, for_right),
        )
        got_right = shifted(to_left, "x", -1)
        got_left = shifted(to_right, "x", 1)
        (summed,) = down(
            own_hidden,
            down_own,
            down_other,
            f,
            ((((0, 0), (1, 0)), ((0, 1), (1, 1))),),
            (got_left, got_right),
            split=z_count,
        )
        backs.append(exchanged(summed).reshape(tok_rows * TOPK, -1))

    own_map = lax.dynamic_slice_in_dim(sample_map, own_device * SAMP_DEV, SAMP_DEV)
    dest_dp = own_map // SAMP_DEV // x_count
    sample_ids = jnp.arange(SAMP_DEV, dtype=jnp.int32)
    goes = dest_dp[None, :] == jnp.arange(dp_count, dtype=jnp.int32)[:, None]
    slot_sample = jnp.sum(jnp.where(goes, sample_ids[None, :], 0), axis=1)
    own_places = own_device * SAMP_DEV + sample_ids
    sources = jnp.sum(
        jnp.where(
            sample_map[None, :] == own_places[:, None],
            jnp.arange(sample_map.shape[0], dtype=jnp.int32)[None, :],
            0,
        ),
        axis=1,
    )
    source_dp = sources // SAMP_DEV // x_count

    sent = jnp.concatenate(
        [
            cache.reshape(SAMP_DEV, 1, ROWS, width)[slot_sample]
            for cache in (out_cache[0], in_cache[0])
        ],
        axis=1,
    )
    sent, _ = lax.optimization_barrier((sent, blocks[1]))
    got = lax.all_to_all(sent, ("z", "core"), split_axis=0, concat_axis=0, tiled=True)
    moved = got[source_dp]
    out_moved = moved[:, 0].reshape(tok_rows, width)
    in_moved = moved[:, 1].reshape(tok_rows, width)

    live = (
        jnp.arange(tok_rows, dtype=jnp.int32) % ROWS < jnp.repeat(lengths, ROWS)
    ).astype(jnp.int32)[:, None]
    slot = slot.T
    sections = lax.axis_size("section")
    caches, arrivals = [], []
    part = width // FEATURE_CHUNKS
    for f, back in enumerate(backs):
        columns = out_moved[:, f * part : (f + 1) * part]
        delta, cache = combine(back, slot, gate_table[0], live, columns)
        caches.append(cache)
        arrivals.append(lax.ppermute(delta, "section", [(i, i + 1) for i in range(sections - 1)]))
    new_out = jnp.concatenate(caches, axis=1)
    received = jnp.concatenate(arrivals, axis=1)
    next_input = (in_moved.astype(F32) + received.astype(F32)).astype(BF16)
    return next_input[None], new_out[None]


def solution(mesh):
    sections, dp, expert = mesh.devices.shape
    split = Mesh(
        mesh.devices.reshape(sections, dp // 2, 2, expert), ("section", "z", "core", "x")
    )
    group = ("z", "core", "x")
    rows = P("section", group, None)
    placed = (rows, rows, rows, P("section", None, group), rows, rows, rows, P(group), P())
    return jax.shard_map(
        section_step, mesh=split, in_specs=placed, out_specs=(rows, rows), check_vma=False
    )
```

```python
import functools

import jax
import jax.numpy as jnp
from jax import lax
from jax.experimental import pallas as pl
from jax.experimental.pallas import tpu as pltpu
from jax.sharding import Mesh, PartitionSpec as P

EXPERTS = 8
TOPK = 2
ROWS = 16
SAMP_DEV = 8
ROW_CHUNKS = 2
FEATURE_CHUNKS = 2
TILE = 256
SMALL_VMEM = 8 << 20
LARGE_VMEM = 12 << 20
BF16 = jnp.bfloat16
F32 = jnp.float32


def shifted(value, axis, by):
    peers = lax.axis_size(axis)
    return lax.ppermute(value, axis, [(i, (i + by) % peers) for i in range(peers)])


def exchanged(value):
    return lax.all_to_all(value, "z", split_axis=0, concat_axis=0, tiled=True)


def group_kernel(routing_ref, tokens_ref, *out_refs):
    chunk_refs, slot_ref = out_refs[:-1], out_refs[-1]
    rows = tokens_ref.shape[0]
    per_expert = rows * TOPK // EXPERTS
    part = per_expert // ROW_CHUNKS
    experts = lax.broadcasted_iota(jnp.int32, (2 * EXPERTS, rows), 0)
    earlier = (
        lax.broadcasted_iota(jnp.int32, (rows, rows), 0)
        < lax.broadcasted_iota(jnp.int32, (rows, rows), 1)
    ).astype(F32).astype(BF16)
    first = (routing_ref[0:1, :] == experts).astype(F32)
    second = (routing_ref[1:2, :] == experts).astype(F32)
    before_first = jnp.dot(first.astype(BF16), earlier, preferred_element_type=F32)
    before_second = jnp.dot(second.astype(BF16), earlier, preferred_element_type=F32) + jnp.sum(
        first, axis=1, keepdims=True
    )
    base = (experts * per_expert).astype(F32)
    slot_first = jnp.sum(first * (before_first + base), axis=0, keepdims=True).astype(jnp.int32)
    slot_second = jnp.sum(second * (before_second + base), axis=0, keepdims=True).astype(jnp.int32)
    slot_ref[0:1, :] = slot_first
    slot_ref[1:2, :] = slot_second
    tokens = tokens_ref[...]
    index = lax.broadcasted_iota(jnp.int32, (EXPERTS * part, rows), 0)
    for chunk, chunk_ref in enumerate(chunk_refs):
        wanted = index // part * per_expert + chunk * part + index % part
        chosen = ((slot_first == wanted) | (slot_second == wanted)).astype(F32).astype(BF16)
        chunk_ref[...] = jnp.dot(chosen, tokens, preferred_element_type=F32).astype(BF16)


def group_rows(routing, tokens):
    rows, width = tokens.shape
    slots = rows * TOPK
    chunk = jax.ShapeDtypeStruct((slots // ROW_CHUNKS, width), BF16)
    out = pl.pallas_call(
        group_kernel,
        out_shape=(chunk,) * ROW_CHUNKS + (jax.ShapeDtypeStruct((TOPK, rows), jnp.int32),),
        compiler_params=pltpu.CompilerParams(vmem_limit_bytes=SMALL_VMEM),
        cost_estimate=pl.CostEstimate(
            flops=2 * slots * rows * width, bytes_accessed=3 * slots * width, transcendentals=0
        ),
        name="group_rows",
    )(routing, tokens)
    return out[:-1], out[-1]


def stage_kernel(own_ref, other_ref, own_out_ref, other_out_ref, sems):
    copies = [
        pltpu.make_async_copy(own_ref, own_out_ref, sems.at[0]),
        pltpu.make_async_copy(other_ref, other_out_ref, sems.at[1]),
    ]
    for copy in copies:
        copy.start()
    for copy in copies:
        copy.wait()


def stage(own, other):
    return pl.pallas_call(
        stage_kernel,
        in_specs=[pl.BlockSpec(memory_space=pl.ANY)] * 2,
        out_specs=[pl.BlockSpec(memory_space=pltpu.VMEM)] * 2,
        out_shape=[jax.ShapeDtypeStruct(own.shape, BF16)] * 2,
        scratch_shapes=[pltpu.SemaphoreType.DMA((2,))],
        compiler_params=pltpu.CompilerParams(vmem_limit_bytes=LARGE_VMEM),
        cost_estimate=pl.CostEstimate(
            flops=1000000, bytes_accessed=8 * own.size, transcendentals=0
        ),
    )(own, other)


def beside(first_ref, second_ref, start, stop):
    width = first_ref.shape[1]
    if stop <= width:
        return first_ref[:, start:stop]
    if start >= width:
        return second_ref[:, start - width : stop - width]
    return jnp.concatenate([first_ref[:, start:], second_ref[:, : stop - width]], axis=1)


def up_kernel(count, *refs):
    row_refs, own_ref, other_ref, out_refs = refs[:count], refs[count], refs[count + 1], refs[count + 2 :]
    rows = jnp.concatenate([ref[...] for ref in row_refs], axis=0)
    for start in range(0, 2 * own_ref.shape[1], TILE):
        weights = beside(own_ref, other_ref, start, start + TILE)
        value = jnp.dot(rows, weights, preferred_element_type=F32)
        hidden = (value / (1.0 + jnp.exp(-value))).astype(BF16)
        at = 0
        for ref in out_refs:
            ref[:, start : start + TILE] = hidden[at : at + ref.shape[0]]
            at += ref.shape[0]


def up(blocks, own, other):
    depth, units = own.shape
    total = sum(block.shape[0] for block in blocks)
    return pl.pallas_call(
        functools.partial(up_kernel, len(blocks)),
        out_shape=[jax.ShapeDtypeStruct((block.shape[0], 2 * units), BF16) for block in blocks],
        compiler_params=pltpu.CompilerParams(vmem_limit_bytes=LARGE_VMEM),
        cost_estimate=pl.CostEstimate(
            flops=4 * total * depth * units,
            bytes_accessed=4 * depth * units + 2 * total * depth,
            transcendentals=2 * total * units,
        ),
    )(*blocks, own, other)


def down_kernel(count, chunk, added, split, *refs):
    hidden_refs, own_ref, other_ref = refs[:count], refs[count], refs[count + 1]
    extra_refs = refs[count + 2 : len(refs) - len(added)]
    out_refs = refs[len(refs) - len(added) :]
    hidden = jnp.concatenate([ref[...] for ref in hidden_refs], axis=0)
    rows = hidden_refs[0].shape[0]
    width = out_refs[0].shape[-1]
    for start in range(0, width, TILE):
        here = slice(start, start + TILE)
        there = slice(chunk * width + start, chunk * width + start + TILE)
        weights = jnp.concatenate([own_ref[:, there], other_ref[:, there]], axis=0)
        term = jnp.dot(hidden, weights, preferred_element_type=F32)
        at = 0
        for parts, out_ref in zip(added, out_refs):
            for number, operands in enumerate(parts):
                value = term[at : at + rows]
                for which, lead in operands:
                    extra = extra_refs[which]
                    value += (extra[:, here] if lead is None else extra[lead, :, here]).astype(F32)
                value = value.astype(BF16)
                if split:
                    out_ref[:, number, :, here] = value.reshape(split, rows // split, TILE)
                elif len(parts) == 1:
                    out_ref[:, here] = value
                else:
                    out_ref[number, :, here] = value
                at += rows


def down(hidden, own, other, chunk, added, extras=(), split=0):
    rows, units = hidden[0].shape
    units //= 2
    width = own.shape[1] // FEATURE_CHUNKS
    out_shape = []
    for parts in added:
        if split:
            lead = (split, len(parts), rows // split)
        elif len(parts) == 1:
            lead = (rows,)
        else:
            lead = (len(parts), rows)
        out_shape.append(jax.ShapeDtypeStruct(lead + (width,), BF16))
    total = rows * len(hidden)
    return pl.pallas_call(
        functools.partial(down_kernel, len(hidden), chunk, added, split),
        out_shape=out_shape,
        compiler_params=pltpu.CompilerParams(vmem_limit_bytes=LARGE_VMEM),
        cost_estimate=pl.CostEstimate(
            flops=4 * total * width * units,
            bytes_accessed=4 * width * units + 2 * total * width,
            transcendentals=0,
        ),
    )(*hidden, own, other, *extras)


def combine_kernel(slot_ref, gate_ref, live_ref, moved_ref, back_ref, delta_ref, cache_ref):
    rows = slot_ref.shape[0]
    back = back_ref[...]
    slots = back.shape[0]
    slot_lanes = lax.broadcasted_iota(jnp.int32, (rows, slots), 1)
    slot = slot_ref[...]
    pick_first = (slot[:, 0:1] == slot_lanes).astype(F32).astype(BF16)
    pick_second = (slot[:, 1:2] == slot_lanes).astype(F32).astype(BF16)
    first = jnp.dot(pick_first, back, preferred_element_type=F32)
    second = jnp.dot(pick_second, back, preferred_element_type=F32)
    gates = gate_ref[...].astype(F32)
    total = gates[:, 0:1] + gates[:, 1:2]
    mixed = gates[:, 0:1] / total * first + gates[:, 1:2] / total * second
    moved = moved_ref[...].astype(F32)
    delta = jnp.where(live_ref[...] > 0, mixed - moved, 0.0).astype(BF16)
    delta_ref[...] = delta
    cache_ref[...] = (moved + delta.astype(F32)).astype(BF16)


def combine(back, slot, gates, live, moved):
    rows, width = moved.shape
    out = jax.ShapeDtypeStruct((rows, width), BF16)
    return pl.pallas_call(
        combine_kernel,
        out_shape=(out, out),
        compiler_params=pltpu.CompilerParams(vmem_limit_bytes=SMALL_VMEM),
        cost_estimate=pl.CostEstimate(
            flops=4 * TOPK * rows * rows * width,
            bytes_accessed=(2 * TOPK + 6) * moved.size,
            transcendentals=0,
        ),
    )(slot, gates, live, moved, back)


def section_step(
    inputs, in_cache, out_cache, w_up, w_down, routing, gate_table, lengths, sample_map
):
    width = inputs.shape[2]
    tok_rows = inputs.shape[1]
    z_count = lax.axis_size("z")
    x_count = lax.axis_size("x")
    dp_count = z_count * lax.axis_size("core")
    own_dp = lax.axis_index(("z", "core"))
    own_device = own_dp * x_count + lax.axis_index("x")

    chunks, slot = group_rows(routing[0].T, inputs[0])
    up_own, down_own = w_up[0], w_down[0]
    blocks = [exchanged(chunk.reshape(z_count, -1, width)).reshape(-1, width) for chunk in chunks]
    up_other = shifted(up_own, "core", 1)
    down_other = shifted(down_own, "core", 1)
    up_own, up_other = stage(up_own, up_other)
    down_own, down_other = stage(down_own, down_other)
    from_left = [shifted(block, "x", 1) for block in blocks]
    from_right = [shifted(block, "x", -1) for block in blocks]
    far = [shifted(from_left[0], "x", 1), shifted(from_right[1], "x", -1)]
    near_hidden = [
        up([blocks[c], from_left[c], from_right[c]], up_own, up_other)
        for c in range(ROW_CHUNKS)
    ]
    far_hidden = up(far, up_own, up_other)
    own_hidden = [hidden[0] for hidden in near_hidden]
    side_hidden = [hidden[1] for hidden in near_hidden] + [hidden[2] for hidden in near_hidden]

    backs = []
    for f in range(FEATURE_CHUNKS):
        far_first, far_second = down(far_hidden, down_own, down_other, f, (((),), ((),)))
        for_left = shifted(far_first, "x", -1)
        for_right = shifted(far_second, "x", 1)
        to_left, to_right = down(
            side_hidden,
            down_own,
            down_other,
            f,
            ((((0, None),), ()), ((), ((1, None),))),
            (for_left, for_right),
        )
        got_right = shifted(to_left, "x", -1)
        got_left = shifted(to_right, "x", 1)
        (summed,) = down(
            own_hidden,
            down_own,
            down_other,
            f,
            ((((0, 0), (1, 0)), ((0, 1), (1, 1))),),
            (got_left, got_right),
            split=z_count,
        )
        backs.append(exchanged(summed).reshape(tok_rows * TOPK, -1))

    own_map = lax.dynamic_slice_in_dim(sample_map, own_device * SAMP_DEV, SAMP_DEV)
    dest_dp = own_map // SAMP_DEV // x_count
    sample_ids = jnp.arange(SAMP_DEV, dtype=jnp.int32)
    goes = dest_dp[None, :] == jnp.arange(dp_count, dtype=jnp.int32)[:, None]
    slot_sample = jnp.sum(jnp.where(goes, sample_ids[None, :], 0), axis=1)
    own_places = own_device * SAMP_DEV + sample_ids
    sources = jnp.sum(
        jnp.where(
            sample_map[None, :] == own_places[:, None],
            jnp.arange(sample_map.shape[0], dtype=jnp.int32)[None, :],
            0,
        ),
        axis=1,
    )
    source_dp = sources // SAMP_DEV // x_count

    sent = jnp.concatenate(
        [
            cache.reshape(SAMP_DEV, 1, ROWS, width)[slot_sample]
            for cache in (out_cache[0], in_cache[0])
        ],
        axis=1,
    )
    sent, _ = lax.optimization_barrier((sent, blocks[1]))
    got = lax.all_to_all(sent, ("z", "core"), split_axis=0, concat_axis=0, tiled=True)
    moved = got[source_dp]
    out_moved = moved[:, 0].reshape(tok_rows, width)
    in_moved = moved[:, 1].reshape(tok_rows, width)

    live = (
        jnp.arange(tok_rows, dtype=jnp.int32) % ROWS < jnp.repeat(lengths, ROWS)
    ).astype(jnp.int32)[:, None]
    slot = slot.T
    sections = lax.axis_size("section")
    caches, arrivals = [], []
    part = width // FEATURE_CHUNKS
    for f, back in enumerate(backs):
        columns = out_moved[:, f * part : (f + 1) * part]
        delta, cache = combine(back, slot, gate_table[0], live, columns)
        caches.append(cache)
        arrivals.append(lax.ppermute(delta, "section", [(i, i + 1) for i in range(sections - 1)]))
    new_out = jnp.concatenate(caches, axis=1)
    received = jnp.concatenate(arrivals, axis=1)
    next_input = (in_moved.astype(F32) + received.astype(F32)).astype(BF16)
    return next_input[None], new_out[None]


def solution(mesh):
    sections, dp, expert = mesh.devices.shape
    split = Mesh(
        mesh.devices.reshape(sections, dp // 2, 2, expert), ("section", "z", "core", "x")
    )
    group = ("z", "core", "x")
    rows = P("section", group, None)
    placed = (rows, rows, rows, P("section", None, group), rows, rows, rows, P(group), P())
    return jax.shard_map(
        section_step, mesh=split, in_specs=placed, out_specs=(rows, rows), check_vma=False
    )
```

```python
import functools

import jax
import jax.numpy as jnp
from jax import lax
from jax.experimental import pallas as pl
from jax.experimental.pallas import tpu as pltpu
from jax.sharding import Mesh, PartitionSpec as P

EXPERTS = 8
TOPK = 2
ROWS = 16
SAMP_DEV = 8
ROW_CHUNKS = 2
FEATURE_CHUNKS = 2
TILE = 256
SMALL_VMEM = 8 << 20
LARGE_VMEM = 12 << 20
BF16 = jnp.bfloat16
F32 = jnp.float32


def shifted(value, axis, by):
    peers = lax.axis_size(axis)
    return lax.ppermute(value, axis, [(i, (i + by) % peers) for i in range(peers)])


def exchanged(value):
    return lax.all_to_all(value, "z", split_axis=0, concat_axis=0, tiled=True)


def group_kernel(routing_ref, tokens_ref, *out_refs):
    chunk_refs, slot_ref = out_refs[:-1], out_refs[-1]
    rows = tokens_ref.shape[0]
    per_expert = rows * TOPK // EXPERTS
    part = per_expert // ROW_CHUNKS
    experts = lax.broadcasted_iota(jnp.int32, (2 * EXPERTS, rows), 0)
    earlier = (
        lax.broadcasted_iota(jnp.int32, (rows, rows), 0)
        < lax.broadcasted_iota(jnp.int32, (rows, rows), 1)
    ).astype(F32).astype(BF16)
    first = (routing_ref[0:1, :] == experts).astype(F32)
    second = (routing_ref[1:2, :] == experts).astype(F32)
    before_first = jnp.dot(first.astype(BF16), earlier, preferred_element_type=F32)
    before_second = jnp.dot(second.astype(BF16), earlier, preferred_element_type=F32) + jnp.sum(
        first, axis=1, keepdims=True
    )
    base = (experts * per_expert).astype(F32)
    slot_first = jnp.sum(first * (before_first + base), axis=0, keepdims=True).astype(jnp.int32)
    slot_second = jnp.sum(second * (before_second + base), axis=0, keepdims=True).astype(jnp.int32)
    slot_ref[0:1, :] = slot_first
    slot_ref[1:2, :] = slot_second
    tokens = tokens_ref[...]
    index = lax.broadcasted_iota(jnp.int32, (EXPERTS * part, rows), 0)
    for chunk, chunk_ref in enumerate(chunk_refs):
        wanted = index // part * per_expert + chunk * part + index % part
        chosen = ((slot_first == wanted) | (slot_second == wanted)).astype(F32).astype(BF16)
        chunk_ref[...] = jnp.dot(chosen, tokens, preferred_element_type=F32).astype(BF16)


def group_rows(routing, tokens):
    rows, width = tokens.shape
    slots = rows * TOPK
    chunk = jax.ShapeDtypeStruct((slots // ROW_CHUNKS, width), BF16)
    out = pl.pallas_call(
        group_kernel,
        out_shape=(chunk,) * ROW_CHUNKS + (jax.ShapeDtypeStruct((TOPK, rows), jnp.int32),),
        compiler_params=pltpu.CompilerParams(vmem_limit_bytes=SMALL_VMEM),
        cost_estimate=pl.CostEstimate(
            flops=2 * slots * rows * width, bytes_accessed=3 * slots * width, transcendentals=0
        ),
        name="group_rows",
    )(routing, tokens)
    return out[:-1], out[-1]


def stage_kernel(own_ref, other_ref, own_out_ref, other_out_ref, sems):
    copies = [
        pltpu.make_async_copy(own_ref, own_out_ref, sems.at[0]),
        pltpu.make_async_copy(other_ref, other_out_ref, sems.at[1]),
    ]
    for copy in copies:
        copy.start()
    for copy in copies:
        copy.wait()


def stage(own, other):
    return pl.pallas_call(
        stage_kernel,
        in_specs=[pl.BlockSpec(memory_space=pl.ANY)] * 2,
        out_specs=[pl.BlockSpec(memory_space=pltpu.VMEM)] * 2,
        out_shape=[jax.ShapeDtypeStruct(own.shape, BF16)] * 2,
        scratch_shapes=[pltpu.SemaphoreType.DMA((2,))],
        compiler_params=pltpu.CompilerParams(vmem_limit_bytes=LARGE_VMEM),
        cost_estimate=pl.CostEstimate(
            flops=1000000, bytes_accessed=8 * own.size, transcendentals=0
        ),
    )(own, other)


def beside(first_ref, second_ref, start, stop):
    width = first_ref.shape[1]
    if stop <= width:
        return first_ref[:, start:stop]
    if start >= width:
        return second_ref[:, start - width : stop - width]
    return jnp.concatenate([first_ref[:, start:], second_ref[:, : stop - width]], axis=1)


def up_kernel(count, *refs):
    row_refs, own_ref, other_ref, out_refs = refs[:count], refs[count], refs[count + 1], refs[count + 2 :]
    rows = jnp.concatenate([ref[...] for ref in row_refs], axis=0)
    for start in range(0, 2 * own_ref.shape[1], TILE):
        weights = beside(own_ref, other_ref, start, start + TILE)
        value = jnp.dot(rows, weights, preferred_element_type=F32)
        hidden = (value / (1.0 + jnp.exp(-value))).astype(BF16)
        at = 0
        for ref in out_refs:
            ref[:, start : start + TILE] = hidden[at : at + ref.shape[0]]
            at += ref.shape[0]


def up(blocks, own, other):
    depth, units = own.shape
    total = sum(block.shape[0] for block in blocks)
    return pl.pallas_call(
        functools.partial(up_kernel, len(blocks)),
        out_shape=[jax.ShapeDtypeStruct((block.shape[0], 2 * units), BF16) for block in blocks],
        compiler_params=pltpu.CompilerParams(vmem_limit_bytes=LARGE_VMEM),
        cost_estimate=pl.CostEstimate(
            flops=4 * total * depth * units,
            bytes_accessed=4 * depth * units + 2 * total * depth,
            transcendentals=2 * total * units,
        ),
    )(*blocks, own, other)


def down_kernel(count, chunk, added, split, *refs):
    hidden_refs, own_ref, other_ref = refs[:count], refs[count], refs[count + 1]
    extra_refs = refs[count + 2 : len(refs) - len(added)]
    out_refs = refs[len(refs) - len(added) :]
    hidden = jnp.concatenate([ref[...] for ref in hidden_refs], axis=0)
    rows = hidden_refs[0].shape[0]
    width = out_refs[0].shape[-1]
    for start in range(0, width, TILE):
        here = slice(start, start + TILE)
        there = slice(chunk * width + start, chunk * width + start + TILE)
        weights = jnp.concatenate([own_ref[:, there], other_ref[:, there]], axis=0)
        term = jnp.dot(hidden, weights, preferred_element_type=F32)
        at = 0
        for parts, out_ref in zip(added, out_refs):
            for number, operands in enumerate(parts):
                value = term[at : at + rows]
                for which, lead in operands:
                    extra = extra_refs[which]
                    value += (extra[:, here] if lead is None else extra[lead, :, here]).astype(F32)
                value = value.astype(BF16)
                if split:
                    out_ref[:, number, :, here] = value.reshape(split, rows // split, TILE)
                elif len(parts) == 1:
                    out_ref[:, here] = value
                else:
                    out_ref[number, :, here] = value
                at += rows


def down(hidden, own, other, chunk, added, extras=(), split=0):
    rows, units = hidden[0].shape
    units //= 2
    width = own.shape[1] // FEATURE_CHUNKS
    out_shape = []
    for parts in added:
        if split:
            lead = (split, len(parts), rows // split)
        elif len(parts) == 1:
            lead = (rows,)
        else:
            lead = (len(parts), rows)
        out_shape.append(jax.ShapeDtypeStruct(lead + (width,), BF16))
    total = rows * len(hidden)
    return pl.pallas_call(
        functools.partial(down_kernel, len(hidden), chunk, added, split),
        out_shape=out_shape,
        compiler_params=pltpu.CompilerParams(vmem_limit_bytes=LARGE_VMEM),
        cost_estimate=pl.CostEstimate(
            flops=4 * total * width * units,
            bytes_accessed=4 * width * units + 2 * total * width,
            transcendentals=0,
        ),
    )(*hidden, own, other, *extras)


def combine_kernel(slot_ref, gate_ref, live_ref, moved_ref, back_ref, delta_ref, cache_ref):
    rows = slot_ref.shape[0]
    back = back_ref[...]
    slots = back.shape[0]
    slot_lanes = lax.broadcasted_iota(jnp.int32, (rows, slots), 1)
    slot = slot_ref[...]
    pick_first = (slot[:, 0:1] == slot_lanes).astype(F32).astype(BF16)
    pick_second = (slot[:, 1:2] == slot_lanes).astype(F32).astype(BF16)
    first = jnp.dot(pick_first, back, preferred_element_type=F32)
    second = jnp.dot(pick_second, back, preferred_element_type=F32)
    gates = gate_ref[...].astype(F32)
    total = gates[:, 0:1] + gates[:, 1:2]
    mixed = gates[:, 0:1] / total * first + gates[:, 1:2] / total * second
    moved = moved_ref[...].astype(F32)
    delta = jnp.where(live_ref[...] > 0, mixed - moved, 0.0).astype(BF16)
    delta_ref[...] = delta
    cache_ref[...] = (moved + delta.astype(F32)).astype(BF16)


def combine(back, slot, gates, live, moved):
    rows, width = moved.shape
    out = jax.ShapeDtypeStruct((rows, width), BF16)
    return pl.pallas_call(
        combine_kernel,
        out_shape=(out, out),
        compiler_params=pltpu.CompilerParams(vmem_limit_bytes=SMALL_VMEM),
        cost_estimate=pl.CostEstimate(
            flops=4 * TOPK * rows * rows * width,
            bytes_accessed=(2 * TOPK + 6) * moved.size,
            transcendentals=0,
        ),
    )(slot, gates, live, moved, back)


def section_step(
    inputs, in_cache, out_cache, w_up, w_down, routing, gate_table, lengths, sample_map
):
    width = inputs.shape[2]
    tok_rows = inputs.shape[1]
    z_count = lax.axis_size("z")
    x_count = lax.axis_size("x")
    dp_count = z_count * lax.axis_size("core")
    own_dp = lax.axis_index(("z", "core"))
    own_device = own_dp * x_count + lax.axis_index("x")

    chunks, slot = group_rows(routing[0].T, inputs[0])
    up_own, down_own = w_up[0], w_down[0]
    blocks = [exchanged(chunk.reshape(z_count, -1, width)).reshape(-1, width) for chunk in chunks]
    up_other = shifted(up_own, "core", 1)
    down_other = shifted(down_own, "core", 1)
    up_own, up_other = stage(up_own, up_other)
    down_own, down_other = stage(down_own, down_other)
    from_left = [shifted(block, "x", 1) for block in blocks]
    from_right = [shifted(block, "x", -1) for block in blocks]
    far = [shifted(from_left[0], "x", 1), shifted(from_right[1], "x", -1)]
    near_hidden = [
        up([blocks[c], from_left[c], from_right[c]], up_own, up_other)
        for c in range(ROW_CHUNKS)
    ]
    far_hidden = up(far, up_own, up_other)
    own_hidden = [hidden[0] for hidden in near_hidden]
    side_hidden = [hidden[1] for hidden in near_hidden] + [hidden[2] for hidden in near_hidden]

    backs = []
    for f in range(FEATURE_CHUNKS):
        to_left, to_right = down(side_hidden, down_own, down_other, f, (((), ()), ((), ())))
        got_right = shifted(to_left, "x", -1)
        got_left = shifted(to_right, "x", 1)
        (to_far,) = down(far_hidden, down_own, down_other, f, (((), ()),))
        got_far = shifted(to_far, "x", 2)
        (summed,) = down(
            own_hidden,
            down_own,
            down_other,
            f,
            (tuple(tuple((which, c) for which in range(3)) for c in range(ROW_CHUNKS)),),
            (got_left, got_right, got_far),
            split=z_count,
        )
        backs.append(exchanged(summed).reshape(tok_rows * TOPK, -1))

    own_map = lax.dynamic_slice_in_dim(sample_map, own_device * SAMP_DEV, SAMP_DEV)
    dest_dp = own_map // SAMP_DEV // x_count
    sample_ids = jnp.arange(SAMP_DEV, dtype=jnp.int32)
    goes = dest_dp[None, :] == jnp.arange(dp_count, dtype=jnp.int32)[:, None]
    slot_sample = jnp.sum(jnp.where(goes, sample_ids[None, :], 0), axis=1)
    own_places = own_device * SAMP_DEV + sample_ids
    sources = jnp.sum(
        jnp.where(
            sample_map[None, :] == own_places[:, None],
            jnp.arange(sample_map.shape[0], dtype=jnp.int32)[None, :],
            0,
        ),
        axis=1,
    )
    source_dp = sources // SAMP_DEV // x_count

    sent = jnp.concatenate(
        [
            cache.reshape(SAMP_DEV, 1, ROWS, width)[slot_sample]
            for cache in (out_cache[0], in_cache[0])
        ],
        axis=1,
    )
    sent, _ = lax.optimization_barrier((sent, blocks[1]))
    got = lax.all_to_all(sent, ("z", "core"), split_axis=0, concat_axis=0, tiled=True)
    moved = got[source_dp]
    out_moved = moved[:, 0].reshape(tok_rows, width)
    in_moved = moved[:, 1].reshape(tok_rows, width)

    live = (
        jnp.arange(tok_rows, dtype=jnp.int32) % ROWS < jnp.repeat(lengths, ROWS)
    ).astype(jnp.int32)[:, None]
    slot = slot.T
    sections = lax.axis_size("section")
    caches, arrivals = [], []
    part = width // FEATURE_CHUNKS
    for f, back in enumerate(backs):
        columns = out_moved[:, f * part : (f + 1) * part]
        delta, cache = combine(back, slot, gate_table[0], live, columns)
        caches.append(cache)
        arrivals.append(lax.ppermute(delta, "section", [(i, i + 1) for i in range(sections - 1)]))
    new_out = jnp.concatenate(caches, axis=1)
    received = jnp.concatenate(arrivals, axis=1)
    next_input = (in_moved.astype(F32) + received.astype(F32)).astype(BF16)
    return next_input[None], new_out[None]


def solution(mesh):
    sections, dp, expert = mesh.devices.shape
    split = Mesh(
        mesh.devices.reshape(sections, dp // 2, 2, expert), ("section", "z", "core", "x")
    )
    group = ("z", "core", "x")
    rows = P("section", group, None)
    placed = (rows, rows, rows, P("section", None, group), rows, rows, rows, P(group), P())
    return jax.shard_map(
        section_step, mesh=split, in_specs=placed, out_specs=(rows, rows), check_vma=False
    )
```

```python
import functools

import jax
import jax.numpy as jnp
from jax import lax
from jax.experimental import pallas as pl
from jax.experimental.pallas import tpu as pltpu
from jax.sharding import Mesh, PartitionSpec as P

EXPERTS = 8
TOPK = 2
ROWS = 16
SAMP_DEV = 8
ROW_CHUNKS = 2
FEATURE_CHUNKS = 2
TILE = 256
SMALL_VMEM = 8 << 20
LARGE_VMEM = 12 << 20
BF16 = jnp.bfloat16
F32 = jnp.float32


def shifted(value, axis, by):
    peers = lax.axis_size(axis)
    return lax.ppermute(value, axis, [(i, (i + by) % peers) for i in range(peers)])


def exchanged(value):
    return lax.all_to_all(value, "z", split_axis=0, concat_axis=0, tiled=True)


def group_kernel(routing_ref, tokens_ref, *out_refs):
    chunk_refs, slot_ref = out_refs[:-1], out_refs[-1]
    rows = tokens_ref.shape[0]
    per_expert = rows * TOPK // EXPERTS
    part = per_expert // ROW_CHUNKS
    experts = lax.broadcasted_iota(jnp.int32, (2 * EXPERTS, rows), 0)
    earlier = (
        lax.broadcasted_iota(jnp.int32, (rows, rows), 0)
        < lax.broadcasted_iota(jnp.int32, (rows, rows), 1)
    ).astype(F32).astype(BF16)
    first = (routing_ref[0:1, :] == experts).astype(F32)
    second = (routing_ref[1:2, :] == experts).astype(F32)
    before_first = jnp.dot(first.astype(BF16), earlier, preferred_element_type=F32)
    before_second = jnp.dot(second.astype(BF16), earlier, preferred_element_type=F32) + jnp.sum(
        first, axis=1, keepdims=True
    )
    base = (experts * per_expert).astype(F32)
    slot_first = jnp.sum(first * (before_first + base), axis=0, keepdims=True).astype(jnp.int32)
    slot_second = jnp.sum(second * (before_second + base), axis=0, keepdims=True).astype(jnp.int32)
    slot_ref[0:1, :] = slot_first
    slot_ref[1:2, :] = slot_second
    tokens = tokens_ref[...]
    index = lax.broadcasted_iota(jnp.int32, (EXPERTS * part, rows), 0)
    for chunk, chunk_ref in enumerate(chunk_refs):
        wanted = index // part * per_expert + chunk * part + index % part
        chosen = ((slot_first == wanted) | (slot_second == wanted)).astype(F32).astype(BF16)
        chunk_ref[...] = jnp.dot(chosen, tokens, preferred_element_type=F32).astype(BF16)


def group_rows(routing, tokens):
    rows, width = tokens.shape
    slots = rows * TOPK
    chunk = jax.ShapeDtypeStruct((slots // ROW_CHUNKS, width), BF16)
    out = pl.pallas_call(
        group_kernel,
        out_shape=(chunk,) * ROW_CHUNKS + (jax.ShapeDtypeStruct((TOPK, rows), jnp.int32),),
        compiler_params=pltpu.CompilerParams(vmem_limit_bytes=SMALL_VMEM),
        cost_estimate=pl.CostEstimate(
            flops=2 * slots * rows * width, bytes_accessed=3 * slots * width, transcendentals=0
        ),
        name="group_rows",
    )(routing, tokens)
    return out[:-1], out[-1]


def stage_kernel(slice_ref, out_ref, sem):
    copy = pltpu.make_async_copy(slice_ref, out_ref, sem)
    copy.start()
    copy.wait()


def stage(value):
    return pl.pallas_call(
        stage_kernel,
        in_specs=[pl.BlockSpec(memory_space=pltpu.HBM)],
        out_specs=pl.BlockSpec(memory_space=pltpu.VMEM),
        out_shape=jax.ShapeDtypeStruct(value.shape, BF16),
        scratch_shapes=[pltpu.SemaphoreType.DMA],
        compiler_params=pltpu.CompilerParams(vmem_limit_bytes=LARGE_VMEM),
        cost_estimate=pl.CostEstimate(
            flops=1000000, bytes_accessed=4 * value.size, transcendentals=0
        ),
    )(value)


def beside(first_ref, second_ref, start, stop):
    width = first_ref.shape[1]
    if stop <= width:
        return first_ref[:, start:stop]
    if start >= width:
        return second_ref[:, start - width : stop - width]
    return jnp.concatenate([first_ref[:, start:], second_ref[:, : stop - width]], axis=1)


def up_kernel(count, *refs):
    row_refs, own_ref, other_ref, out_refs = refs[:count], refs[count], refs[count + 1], refs[count + 2 :]
    rows = jnp.concatenate([ref[...] for ref in row_refs], axis=0)
    for start in range(0, 2 * own_ref.shape[1], TILE):
        weights = beside(own_ref, other_ref, start, start + TILE)
        value = jnp.dot(rows, weights, preferred_element_type=F32)
        hidden = (value / (1.0 + jnp.exp(-value))).astype(BF16)
        at = 0
        for ref in out_refs:
            ref[:, start : start + TILE] = hidden[at : at + ref.shape[0]]
            at += ref.shape[0]


def up(blocks, own, other):
    depth, units = own.shape
    total = sum(block.shape[0] for block in blocks)
    return pl.pallas_call(
        functools.partial(up_kernel, len(blocks)),
        out_shape=[jax.ShapeDtypeStruct((block.shape[0], 2 * units), BF16) for block in blocks],
        compiler_params=pltpu.CompilerParams(vmem_limit_bytes=LARGE_VMEM),
        cost_estimate=pl.CostEstimate(
            flops=4 * total * depth * units,
            bytes_accessed=4 * depth * units + 2 * total * depth,
            transcendentals=2 * total * units,
        ),
    )(*blocks, own, other)


def down_kernel(count, chunk, added, *refs):
    hidden_refs, own_ref, other_ref = refs[:count], refs[count], refs[count + 1]
    extra_refs = refs[count + 2 : len(refs) - len(added)]
    out_refs = refs[len(refs) - len(added) :]
    hidden = jnp.concatenate([ref[...] for ref in hidden_refs], axis=0)
    rows = hidden_refs[0].shape[0]
    width = out_refs[0].shape[-1]
    for start in range(0, width, TILE):
        here = slice(start, start + TILE)
        there = slice(chunk * width + start, chunk * width + start + TILE)
        weights = jnp.concatenate([own_ref[:, there], other_ref[:, there]], axis=0)
        term = jnp.dot(hidden, weights, preferred_element_type=F32)
        at = 0
        for parts, out_ref in zip(added, out_refs):
            for number, operands in enumerate(parts):
                value = term[at : at + rows]
                for which, lead in operands:
                    extra = extra_refs[which]
                    value += (extra[:, here] if lead is None else extra[lead, :, here]).astype(F32)
                value = value.astype(BF16)
                if len(parts) == 1:
                    out_ref[:, here] = value
                else:
                    out_ref[number, :, here] = value
                at += rows


def down_all_kernel(first_ref, second_ref, own_ref, other_ref, *out_refs):
    hidden = jnp.concatenate([first_ref[...], second_ref[...]], axis=0)
    rows = first_ref.shape[0]
    width = out_refs[0].shape[-1]
    for start in range(0, own_ref.shape[1], TILE):
        out_ref, at = out_refs[start // width], start % width
        there = slice(start, start + TILE)
        weights = jnp.concatenate([own_ref[:, there], other_ref[:, there]], axis=0)
        term = jnp.dot(hidden, weights, preferred_element_type=F32)
        out_ref[0, :, at : at + TILE] = term[:rows]
        out_ref[1, :, at : at + TILE] = term[rows:]


def down_all(hidden, own, other):
    rows = hidden[0].shape[0]
    units, width = own.shape
    out = jax.ShapeDtypeStruct((len(hidden), rows, width // FEATURE_CHUNKS), F32)
    return pl.pallas_call(
        down_all_kernel,
        out_shape=[out] * FEATURE_CHUNKS,
        compiler_params=pltpu.CompilerParams(vmem_limit_bytes=LARGE_VMEM),
        cost_estimate=pl.CostEstimate(
            flops=8 * rows * width * units,
            bytes_accessed=4 * width * units + 8 * rows * width,
            transcendentals=0,
        ),
        name="down_own",
    )(*hidden, own, other)


def total_kernel(own_ref, *refs):
    out_ref = refs[-1]
    groups, parts, rows, _ = out_ref.shape
    for start in range(0, out_ref.shape[-1], TILE):
        here = slice(start, start + TILE)
        for number in range(parts):
            value = own_ref[number, :, here]
            for ref in refs[:-1]:
                value += ref[number, :, here].astype(F32)
            out_ref[:, number, :, here] = value.astype(BF16).reshape(groups, rows, TILE)


def total(own, others, groups):
    parts, rows, width = own.shape
    return pl.pallas_call(
        total_kernel,
        out_shape=jax.ShapeDtypeStruct((groups, parts, rows // groups, width), BF16),
        compiler_params=pltpu.CompilerParams(vmem_limit_bytes=LARGE_VMEM),
        cost_estimate=pl.CostEstimate(
            flops=4 * own.size, bytes_accessed=12 * own.size, transcendentals=0
        ),
    )(own, *others)


def down(hidden, own, other, chunk, added, extras=()):
    rows, units = hidden[0].shape
    units //= 2
    width = own.shape[1] // FEATURE_CHUNKS
    out_shape = []
    for parts in added:
        if len(parts) == 1:
            lead = (rows,)
        else:
            lead = (len(parts), rows)
        out_shape.append(jax.ShapeDtypeStruct(lead + (width,), BF16))
    total = rows * len(hidden)
    return pl.pallas_call(
        functools.partial(down_kernel, len(hidden), chunk, added),
        out_shape=out_shape,
        compiler_params=pltpu.CompilerParams(vmem_limit_bytes=LARGE_VMEM),
        cost_estimate=pl.CostEstimate(
            flops=4 * total * width * units,
            bytes_accessed=4 * width * units + 2 * total * width,
            transcendentals=0,
        ),
    )(*hidden, own, other, *extras)


def combine_kernel(slot_ref, gate_ref, live_ref, moved_ref, back_ref, delta_ref, cache_ref):
    rows = slot_ref.shape[0]
    back = back_ref[...]
    slots = back.shape[0]
    slot_lanes = lax.broadcasted_iota(jnp.int32, (rows, slots), 1)
    slot = slot_ref[...]
    pick_first = (slot[:, 0:1] == slot_lanes).astype(F32).astype(BF16)
    pick_second = (slot[:, 1:2] == slot_lanes).astype(F32).astype(BF16)
    first = jnp.dot(pick_first, back, preferred_element_type=F32)
    second = jnp.dot(pick_second, back, preferred_element_type=F32)
    gates = gate_ref[...].astype(F32)
    total = gates[:, 0:1] + gates[:, 1:2]
    mixed = gates[:, 0:1] / total * first + gates[:, 1:2] / total * second
    moved = moved_ref[...].astype(F32)
    delta = jnp.where(live_ref[...] > 0, mixed - moved, 0.0).astype(BF16)
    delta_ref[...] = delta
    cache_ref[...] = (moved + delta.astype(F32)).astype(BF16)


def combine(back, slot, gates, live, moved):
    rows, width = moved.shape
    out = jax.ShapeDtypeStruct((rows, width), BF16)
    return pl.pallas_call(
        combine_kernel,
        out_shape=(out, out),
        compiler_params=pltpu.CompilerParams(vmem_limit_bytes=SMALL_VMEM),
        cost_estimate=pl.CostEstimate(
            flops=4 * TOPK * rows * rows * width,
            bytes_accessed=(2 * TOPK + 6) * moved.size,
            transcendentals=0,
        ),
    )(slot, gates, live, moved, back)


def section_step(
    inputs, in_cache, out_cache, w_up, w_down, routing, gate_table, lengths, sample_map
):
    width = inputs.shape[2]
    tok_rows = inputs.shape[1]
    z_count = lax.axis_size("z")
    x_count = lax.axis_size("x")
    dp_count = z_count * lax.axis_size("core")
    own_dp = lax.axis_index(("z", "core"))
    own_device = own_dp * x_count + lax.axis_index("x")

    chunks, slot = group_rows(routing[0].T, inputs[0])
    up_own, down_own = w_up[0], w_down[0]
    blocks = [exchanged(chunk.reshape(z_count, -1, width)).reshape(-1, width) for chunk in chunks]
    up_other = shifted(up_own, "core", 1)
    down_other = shifted(down_own, "core", 1)
    up_other, down_other = stage(up_other), stage(down_other)
    from_left = [shifted(block, "x", 1) for block in blocks]
    from_right = [shifted(block, "x", -1) for block in blocks]
    far = [shifted(from_left[0], "x", 1), shifted(from_right[1], "x", -1)]
    near_hidden = [
        up([blocks[c], from_left[c], from_right[c]], up_own, up_other)
        for c in range(ROW_CHUNKS)
    ]
    far_hidden = up(far, up_own, up_other)
    own_hidden = [hidden[0] for hidden in near_hidden]
    side_hidden = [hidden[1] for hidden in near_hidden] + [hidden[2] for hidden in near_hidden]

    own_terms = down_all(own_hidden, down_own, down_other)
    apart = ((), ())
    to_left, to_right = down(side_hidden, down_own, down_other, 0, (apart, apart))
    got_right = shifted(to_left, "x", -1)
    got_left = shifted(to_right, "x", 1)
    (to_far,) = down(far_hidden, down_own, down_other, 0, (apart,))
    got_far = shifted(to_far, "x", 2)
    first_back = total(own_terms[0], (got_left, got_right, got_far), z_count)

    far_first, far_second = down(far_hidden, down_own, down_other, 1, (((),), ((),)))
    for_left = shifted(far_first, "x", -1)
    for_right = shifted(far_second, "x", 1)
    to_left, to_right = down(
        side_hidden,
        down_own,
        down_other,
        1,
        ((((0, None),), ()), ((), ((1, None),))),
        (for_left, for_right),
    )
    got_right = shifted(to_left, "x", -1)
    got_left = shifted(to_right, "x", 1)
    second_back = total(own_terms[1], (got_left, got_right), z_count)
    backs = [exchanged(summed).reshape(tok_rows * TOPK, -1) for summed in (first_back, second_back)]

    own_map = lax.dynamic_slice_in_dim(sample_map, own_device * SAMP_DEV, SAMP_DEV)
    dest_dp = own_map // SAMP_DEV // x_count
    sample_ids = jnp.arange(SAMP_DEV, dtype=jnp.int32)
    goes = dest_dp[None, :] == jnp.arange(dp_count, dtype=jnp.int32)[:, None]
    slot_sample = jnp.sum(jnp.where(goes, sample_ids[None, :], 0), axis=1)
    own_places = own_device * SAMP_DEV + sample_ids
    sources = jnp.sum(
        jnp.where(
            sample_map[None, :] == own_places[:, None],
            jnp.arange(sample_map.shape[0], dtype=jnp.int32)[None, :],
            0,
        ),
        axis=1,
    )
    source_dp = sources // SAMP_DEV // x_count

    sent = jnp.concatenate(
        [
            cache.reshape(SAMP_DEV, 1, ROWS, width)[slot_sample]
            for cache in (out_cache[0], in_cache[0])
        ],
        axis=1,
    )
    sent, _ = lax.optimization_barrier((sent, blocks[1]))
    got = lax.all_to_all(sent, ("z", "core"), split_axis=0, concat_axis=0, tiled=True)
    moved = got[source_dp]
    out_moved = moved[:, 0].reshape(tok_rows, width)
    in_moved = moved[:, 1].reshape(tok_rows, width)

    live = (
        jnp.arange(tok_rows, dtype=jnp.int32) % ROWS < jnp.repeat(lengths, ROWS)
    ).astype(jnp.int32)[:, None]
    slot = slot.T
    sections = lax.axis_size("section")
    caches, arrivals = [], []
    part = width // FEATURE_CHUNKS
    for f, back in enumerate(backs):
        columns = out_moved[:, f * part : (f + 1) * part]
        delta, cache = combine(back, slot, gate_table[0], live, columns)
        caches.append(cache)
        arrivals.append(lax.ppermute(delta, "section", [(i, i + 1) for i in range(sections - 1)]))
    new_out = jnp.concatenate(caches, axis=1)
    received = jnp.concatenate(arrivals, axis=1)
    next_input = (in_moved.astype(F32) + received.astype(F32)).astype(BF16)
    return next_input[None], new_out[None]


def solution(mesh):
    sections, dp, expert = mesh.devices.shape
    split = Mesh(
        mesh.devices.reshape(sections, dp // 2, 2, expert), ("section", "z", "core", "x")
    )
    group = ("z", "core", "x")
    rows = P("section", group, None)
    placed = (rows, rows, rows, P("section", None, group), rows, rows, rows, P(group), P())
    return jax.shard_map(
        section_step, mesh=split, in_specs=placed, out_specs=(rows, rows), check_vma=False
    )
```

```python
import functools

import jax
import jax.numpy as jnp
from jax import lax
from jax.experimental import pallas as pl
from jax.experimental.pallas import tpu as pltpu
from jax.sharding import Mesh, PartitionSpec as P

EXPERTS = 8
TOPK = 2
ROWS = 16
SAMP_DEV = 8
ROW_CHUNKS = 2
FEATURE_CHUNKS = 2
TILE = 256
SMALL_VMEM = 8 << 20
LARGE_VMEM = 12 << 20
BF16 = jnp.bfloat16
F32 = jnp.float32


def shifted(value, axis, by):
    peers = lax.axis_size(axis)
    return lax.ppermute(value, axis, [(i, (i + by) % peers) for i in range(peers)])


def exchanged(value):
    return lax.all_to_all(value, "z", split_axis=0, concat_axis=0, tiled=True)


def group_kernel(plane_ref, routing_ref, tokens_ref, *out_refs):
    chunk_ref, piece_refs, slot_ref = out_refs[0], out_refs[1:-1], out_refs[-1]
    rows = tokens_ref.shape[0]
    per_expert = rows * TOPK // EXPERTS
    part = per_expert // ROW_CHUNKS
    experts = lax.broadcasted_iota(jnp.int32, (2 * EXPERTS, rows), 0)
    earlier = (
        lax.broadcasted_iota(jnp.int32, (rows, rows), 0)
        < lax.broadcasted_iota(jnp.int32, (rows, rows), 1)
    ).astype(F32).astype(BF16)
    first = (routing_ref[0:1, :] == experts).astype(F32)
    second = (routing_ref[1:2, :] == experts).astype(F32)
    before_first = jnp.dot(first.astype(BF16), earlier, preferred_element_type=F32)
    before_second = jnp.dot(second.astype(BF16), earlier, preferred_element_type=F32) + jnp.sum(
        first, axis=1, keepdims=True
    )
    base = (experts * per_expert).astype(F32)
    slot_first = jnp.sum(first * (before_first + base), axis=0, keepdims=True).astype(jnp.int32)
    slot_second = jnp.sum(second * (before_second + base), axis=0, keepdims=True).astype(jnp.int32)
    slot_ref[0:1, :] = slot_first
    slot_ref[1:2, :] = slot_second
    tokens = tokens_ref[...]
    index = lax.broadcasted_iota(jnp.int32, (EXPERTS * part, rows), 0)
    for chunk in range(ROW_CHUNKS):
        expert = index // part
        if chunk:
            expert = (expert + plane_ref[0]) % EXPERTS
        wanted = expert * per_expert + chunk * part + index % part
        chosen = ((slot_first == wanted) | (slot_second == wanted)).astype(F32).astype(BF16)
        picked = jnp.dot(chosen, tokens, preferred_element_type=F32).astype(BF16)
        if chunk:
            for away, ref in enumerate(piece_refs):
                ref[...] = picked[away * part : (away + 1) * part]
        else:
            chunk_ref[...] = picked


def join_kernel(plane_ref, *refs):
    out_ref = refs[-1]
    for away, ref in enumerate(refs[:-1]):
        rows = ref.shape[0]
        source = (plane_ref[0] + EXPERTS - away) % EXPERTS
        out_ref[pl.ds(pl.multiple_of(source * rows, rows), rows), :] = ref[...]


def join(plane, pieces):
    rows, width = pieces[0].shape
    vmem = pl.BlockSpec(memory_space=pltpu.VMEM)
    return pl.pallas_call(
        join_kernel,
        in_specs=[pl.BlockSpec(memory_space=pltpu.SMEM)] + [vmem] * len(pieces),
        out_shape=jax.ShapeDtypeStruct((rows * len(pieces), width), BF16),
        compiler_params=pltpu.CompilerParams(vmem_limit_bytes=SMALL_VMEM),
        cost_estimate=pl.CostEstimate(
            flops=1000000, bytes_accessed=4 * rows * len(pieces) * width, transcendentals=0
        ),
    )(plane, *pieces)


def group_rows(plane, routing, tokens):
    rows, width = tokens.shape
    slots = rows * TOPK
    chunk = jax.ShapeDtypeStruct((slots // ROW_CHUNKS, width), BF16)
    piece = jax.ShapeDtypeStruct((slots // ROW_CHUNKS // EXPERTS, width), BF16)
    vmem = pl.BlockSpec(memory_space=pltpu.VMEM)
    out = pl.pallas_call(
        group_kernel,
        in_specs=[pl.BlockSpec(memory_space=pltpu.SMEM), vmem, vmem],
        out_shape=(chunk,)
        + (piece,) * EXPERTS
        + (jax.ShapeDtypeStruct((TOPK, rows), jnp.int32),),
        compiler_params=pltpu.CompilerParams(vmem_limit_bytes=SMALL_VMEM),
        cost_estimate=pl.CostEstimate(
            flops=2 * slots * rows * width, bytes_accessed=3 * slots * width, transcendentals=0
        ),
        name="group_rows",
    )(plane, routing, tokens)
    return out[0], out[1:-1], out[-1]


def stage_kernel(slice_ref, out_ref, sem):
    copy = pltpu.make_async_copy(slice_ref, out_ref, sem)
    copy.start()
    copy.wait()


def stage(value):
    return pl.pallas_call(
        stage_kernel,
        in_specs=[pl.BlockSpec(memory_space=pltpu.HBM)],
        out_specs=pl.BlockSpec(memory_space=pltpu.VMEM),
        out_shape=jax.ShapeDtypeStruct(value.shape, BF16),
        scratch_shapes=[pltpu.SemaphoreType.DMA],
        compiler_params=pltpu.CompilerParams(vmem_limit_bytes=LARGE_VMEM),
        cost_estimate=pl.CostEstimate(
            flops=1000000, bytes_accessed=4 * value.size, transcendentals=0
        ),
    )(value)


def up_kernel(count, *refs):
    row_refs, own_ref, other_ref, out_refs = refs[:count], refs[count], refs[count + 1], refs[count + 2 :]
    rows = jnp.concatenate([ref[...] for ref in row_refs], axis=0)
    units = own_ref.shape[1]
    left = units % TILE

    def tile(weights, start):
        value = jnp.dot(rows, weights, preferred_element_type=F32)
        hidden = (value / (1.0 + jnp.exp(-value))).astype(BF16)
        at = 0
        for ref in out_refs:
            ref[:, pl.ds(start, TILE)] = hidden[at : at + ref.shape[0]]
            at += ref.shape[0]

    def own_tile(number, carry):
        start = pl.multiple_of(number * TILE, TILE)
        tile(own_ref[:, pl.ds(start, TILE)], start)
        return carry

    def other_tile(number, carry):
        start = pl.multiple_of(number * TILE + TILE - left, TILE // 2)
        tile(other_ref[:, pl.ds(start, TILE)], pl.multiple_of(number * TILE + units + TILE - left, TILE))
        return carry

    lax.fori_loop(0, units // TILE, own_tile, 0)
    tile(
        jnp.concatenate([own_ref[:, units - left :], other_ref[:, : TILE - left]], axis=1),
        units - left,
    )
    lax.fori_loop(0, units // TILE, other_tile, 0)


def up(blocks, own, other):
    depth, units = own.shape
    total = sum(block.shape[0] for block in blocks)
    return pl.pallas_call(
        functools.partial(up_kernel, len(blocks)),
        out_shape=[jax.ShapeDtypeStruct((block.shape[0], 2 * units), BF16) for block in blocks],
        compiler_params=pltpu.CompilerParams(vmem_limit_bytes=LARGE_VMEM),
        cost_estimate=pl.CostEstimate(
            flops=4 * total * depth * units,
            bytes_accessed=4 * depth * units + 2 * total * depth,
            transcendentals=2 * total * units,
        ),
    )(*blocks, own, other)


def down_kernel(count, chunk, added, *refs):
    hidden_refs, own_ref, other_ref = refs[:count], refs[count], refs[count + 1]
    extra_refs = refs[count + 2 : len(refs) - len(added)]
    out_refs = refs[len(refs) - len(added) :]
    hidden = jnp.concatenate([ref[...] for ref in hidden_refs], axis=0)
    rows = hidden_refs[0].shape[0]
    width = out_refs[0].shape[-1]
    for start in range(0, width, TILE):
        here = slice(start, start + TILE)
        there = slice(chunk * width + start, chunk * width + start + TILE)
        weights = jnp.concatenate([own_ref[:, there], other_ref[:, there]], axis=0)
        term = jnp.dot(hidden, weights, preferred_element_type=F32)
        at = 0
        for parts, out_ref in zip(added, out_refs):
            for number, operands in enumerate(parts):
                value = term[at : at + rows]
                for which, lead in operands:
                    extra = extra_refs[which]
                    value += (extra[:, here] if lead is None else extra[lead, :, here]).astype(F32)
                value = value.astype(BF16)
                if len(parts) == 1:
                    out_ref[:, here] = value
                else:
                    out_ref[number, :, here] = value
                at += rows


def down_all_kernel(first_ref, second_ref, own_ref, other_ref, *out_refs):
    hidden = jnp.concatenate([first_ref[...], second_ref[...]], axis=0)
    rows = first_ref.shape[0]
    width = out_refs[0].shape[-1]
    for start in range(0, own_ref.shape[1], TILE):
        out_ref, at = out_refs[start // width], start % width
        there = slice(start, start + TILE)
        weights = jnp.concatenate([own_ref[:, there], other_ref[:, there]], axis=0)
        term = jnp.dot(hidden, weights, preferred_element_type=F32)
        out_ref[0, :, at : at + TILE] = term[:rows]
        out_ref[1, :, at : at + TILE] = term[rows:]


def down_all(hidden, own, other):
    rows = hidden[0].shape[0]
    units, width = own.shape
    out = jax.ShapeDtypeStruct((len(hidden), rows, width // FEATURE_CHUNKS), F32)
    return pl.pallas_call(
        down_all_kernel,
        out_shape=[out] * FEATURE_CHUNKS,
        compiler_params=pltpu.CompilerParams(vmem_limit_bytes=LARGE_VMEM),
        cost_estimate=pl.CostEstimate(
            flops=8 * rows * width * units,
            bytes_accessed=4 * width * units + 8 * rows * width,
            transcendentals=0,
        ),
        name="down_own",
    )(*hidden, own, other)


def total_kernel(own_ref, *refs):
    out_ref = refs[-1]
    groups, parts, rows, _ = out_ref.shape
    for start in range(0, out_ref.shape[-1], TILE):
        here = slice(start, start + TILE)
        for number in range(parts):
            value = own_ref[number, :, here]
            for ref in refs[:-1]:
                value += ref[number, :, here].astype(F32)
            out_ref[:, number, :, here] = value.astype(BF16).reshape(groups, rows, TILE)


def total_pieces_kernel(plane_ref, own_ref, *refs):
    extra_refs, piece_refs, sum_ref = refs[: -EXPERTS - 1], refs[-EXPERTS - 1 : -1], refs[-1]
    parts, rows, width = own_ref.shape
    rows //= EXPERTS
    for start in range(0, width, TILE):
        here = slice(start, start + TILE)
        for number in range(parts):
            value = own_ref[number, :, here]
            for ref in extra_refs:
                value += ref[number, :, here].astype(F32)
            sum_ref[number, :, here] = value.astype(BF16)
    for away, ref in enumerate(piece_refs):
        source = (plane_ref[0] + away) % EXPERTS
        from_rows = pl.ds(pl.multiple_of(source * rows, rows), rows)
        for number in range(parts):
            ref[number * rows : (number + 1) * rows, :] = sum_ref[number, from_rows, :]


def total_pieces(plane, own, others):
    parts, rows, width = own.shape
    vmem = pl.BlockSpec(memory_space=pltpu.VMEM)
    piece = jax.ShapeDtypeStruct((parts * rows // EXPERTS, width), BF16)
    return pl.pallas_call(
        total_pieces_kernel,
        in_specs=[pl.BlockSpec(memory_space=pltpu.SMEM)] + [vmem] * (1 + len(others)),
        out_shape=[piece] * EXPERTS,
        scratch_shapes=[pltpu.VMEM(own.shape, BF16)],
        compiler_params=pltpu.CompilerParams(vmem_limit_bytes=LARGE_VMEM),
        cost_estimate=pl.CostEstimate(
            flops=4 * own.size, bytes_accessed=12 * own.size, transcendentals=0
        ),
    )(plane, own, *others)


def total(own, others, groups):
    parts, rows, width = own.shape
    return pl.pallas_call(
        total_kernel,
        out_shape=jax.ShapeDtypeStruct((groups, parts, rows // groups, width), BF16),
        compiler_params=pltpu.CompilerParams(vmem_limit_bytes=LARGE_VMEM),
        cost_estimate=pl.CostEstimate(
            flops=4 * own.size, bytes_accessed=12 * own.size, transcendentals=0
        ),
    )(own, *others)


def down(hidden, own, other, chunk, added, extras=()):
    rows, units = hidden[0].shape
    units //= 2
    width = own.shape[1] // FEATURE_CHUNKS
    out_shape = []
    for parts in added:
        if len(parts) == 1:
            lead = (rows,)
        else:
            lead = (len(parts), rows)
        out_shape.append(jax.ShapeDtypeStruct(lead + (width,), BF16))
    total = rows * len(hidden)
    return pl.pallas_call(
        functools.partial(down_kernel, len(hidden), chunk, added),
        out_shape=out_shape,
        compiler_params=pltpu.CompilerParams(vmem_limit_bytes=LARGE_VMEM),
        cost_estimate=pl.CostEstimate(
            flops=4 * total * width * units,
            bytes_accessed=4 * width * units + 2 * total * width,
            transcendentals=0,
        ),
    )(*hidden, own, other, *extras)


def combine_kernel(slot_ref, gate_ref, live_ref, moved_ref, *refs):
    back_refs, (delta_ref, cache_ref) = refs[:-2], refs[-2:]
    rows = slot_ref.shape[0]
    back = jnp.concatenate([ref[...] for ref in back_refs], axis=0)
    slots = back.shape[0]
    slot_lanes = lax.broadcasted_iota(jnp.int32, (rows, slots), 1)
    slot = slot_ref[...]
    pick_first = (slot[:, 0:1] == slot_lanes).astype(F32).astype(BF16)
    pick_second = (slot[:, 1:2] == slot_lanes).astype(F32).astype(BF16)
    first = jnp.dot(pick_first, back, preferred_element_type=F32)
    second = jnp.dot(pick_second, back, preferred_element_type=F32)
    gates = gate_ref[...].astype(F32)
    total = gates[:, 0:1] + gates[:, 1:2]
    mixed = gates[:, 0:1] / total * first + gates[:, 1:2] / total * second
    moved = moved_ref[...].astype(F32)
    delta = jnp.where(live_ref[...] > 0, mixed - moved, 0.0).astype(BF16)
    delta_ref[...] = delta
    cache_ref[...] = (moved + delta.astype(F32)).astype(BF16)


def combine(back, slot, gates, live, moved):
    rows, width = moved.shape
    out = jax.ShapeDtypeStruct((rows, width), BF16)
    return pl.pallas_call(
        combine_kernel,
        out_shape=(out, out),
        compiler_params=pltpu.CompilerParams(vmem_limit_bytes=SMALL_VMEM),
        cost_estimate=pl.CostEstimate(
            flops=4 * TOPK * rows * rows * width,
            bytes_accessed=(2 * TOPK + 6) * moved.size,
            transcendentals=0,
        ),
    )(slot, gates, live, moved, *back)


def section_step(
    inputs, in_cache, out_cache, w_up, w_down, routing, gate_table, lengths, sample_map
):
    width = inputs.shape[2]
    tok_rows = inputs.shape[1]
    z_count = lax.axis_size("z")
    x_count = lax.axis_size("x")
    dp_count = z_count * lax.axis_size("core")
    own_dp = lax.axis_index(("z", "core"))
    own_device = own_dp * x_count + lax.axis_index("x")

    plane = lax.axis_index("z").astype(jnp.int32)[None]
    order = sorted(range(1, z_count), key=lambda away: -min(away, z_count - away))
    chunk, pieces, slot = group_rows(plane, routing[0].T, inputs[0])
    up_own, down_own = w_up[0], w_down[0]
    blocks = [exchanged(chunk.reshape(z_count, -1, width)).reshape(-1, width)]
    got = {away: shifted(pieces[away], "z", away) for away in order}
    blocks.append(join(plane, [pieces[0]] + [got[away] for away in range(1, z_count)]))
    up_other = shifted(up_own, "core", 1)
    down_other = shifted(down_own, "core", 1)
    up_other, down_other = stage(up_other), stage(down_other)
    from_left = [shifted(block, "x", 1) for block in blocks]
    from_right = [shifted(block, "x", -1) for block in blocks]
    far = [shifted(from_left[0], "x", 1), shifted(from_right[1], "x", -1)]
    near_hidden = [
        up([blocks[c], from_left[c], from_right[c]], up_own, up_other)
        for c in range(ROW_CHUNKS)
    ]
    far_hidden = up(far, up_own, up_other)
    own_hidden = [hidden[0] for hidden in near_hidden]
    side_hidden = [hidden[1] for hidden in near_hidden] + [hidden[2] for hidden in near_hidden]

    own_terms = down_all(own_hidden, down_own, down_other)
    apart = ((), ())
    to_left, to_right = down(side_hidden, down_own, down_other, 0, (apart, apart))
    got_right = shifted(to_left, "x", -1)
    got_left = shifted(to_right, "x", 1)
    (to_far,) = down(far_hidden, down_own, down_other, 0, (apart,))
    got_far = shifted(to_far, "x", 2)
    first_back = total(own_terms[0], (got_left, got_right, got_far), z_count)

    far_first, far_second = down(far_hidden, down_own, down_other, 1, (((),), ((),)))
    for_left = shifted(far_first, "x", -1)
    for_right = shifted(far_second, "x", 1)
    to_left, to_right = down(
        side_hidden,
        down_own,
        down_other,
        1,
        ((((0, None),), ()), ((), ((1, None),))),
        (for_left, for_right),
    )
    got_right = shifted(to_left, "x", -1)
    got_left = shifted(to_right, "x", 1)
    second_back = total_pieces(plane, own_terms[1], (got_left, got_right))
    got = {away: shifted(second_back[away], "z", away) for away in order}
    backs = [
        [exchanged(first_back).reshape(tok_rows * TOPK, -1)],
        [second_back[0]] + [got[away] for away in range(1, z_count)],
    ]

    own_map = lax.dynamic_slice_in_dim(sample_map, own_device * SAMP_DEV, SAMP_DEV)
    dest_dp = own_map // SAMP_DEV // x_count
    sample_ids = jnp.arange(SAMP_DEV, dtype=jnp.int32)
    goes = dest_dp[None, :] == jnp.arange(dp_count, dtype=jnp.int32)[:, None]
    slot_sample = jnp.sum(jnp.where(goes, sample_ids[None, :], 0), axis=1)
    own_places = own_device * SAMP_DEV + sample_ids
    sources = jnp.sum(
        jnp.where(
            sample_map[None, :] == own_places[:, None],
            jnp.arange(sample_map.shape[0], dtype=jnp.int32)[None, :],
            0,
        ),
        axis=1,
    )
    source_dp = sources // SAMP_DEV // x_count

    sent = jnp.concatenate(
        [
            cache.reshape(SAMP_DEV, 1, ROWS, width)[slot_sample]
            for cache in (out_cache[0], in_cache[0])
        ],
        axis=1,
    )
    sent, _ = lax.optimization_barrier((sent, blocks[1]))
    got = lax.all_to_all(sent, ("z", "core"), split_axis=0, concat_axis=0, tiled=True)
    moved = got[source_dp]
    out_moved = moved[:, 0].reshape(tok_rows, width)
    in_moved = moved[:, 1].reshape(tok_rows, width)

    live = (
        jnp.arange(tok_rows, dtype=jnp.int32) % ROWS < jnp.repeat(lengths, ROWS)
    ).astype(jnp.int32)[:, None]
    slot = slot.T
    per_expert = tok_rows * TOPK // EXPERTS
    behind = (plane[0] + EXPERTS - slot // per_expert) % EXPERTS * per_expert + slot % per_expert
    sections = lax.axis_size("section")
    caches, arrivals = [], []
    part = width // FEATURE_CHUNKS
    for f, back in enumerate(backs):
        columns = out_moved[:, f * part : (f + 1) * part]
        delta, cache = combine(back, behind if f else slot, gate_table[0], live, columns)
        caches.append(cache)
        arrivals.append(lax.ppermute(delta, "section", [(i, i + 1) for i in range(sections - 1)]))
    new_out = jnp.concatenate(caches, axis=1)
    received = jnp.concatenate(arrivals, axis=1)
    next_input = (in_moved.astype(F32) + received.astype(F32)).astype(BF16)
    return next_input[None], new_out[None]


def solution(mesh):
    sections, dp, expert = mesh.devices.shape
    split = Mesh(
        mesh.devices.reshape(sections, dp // 2, 2, expert), ("section", "z", "core", "x")
    )
    group = ("z", "core", "x")
    rows = P("section", group, None)
    placed = (rows, rows, rows, P("section", None, group), rows, rows, rows, P(group), P())
    return jax.shard_map(
        section_step, mesh=split, in_specs=placed, out_specs=(rows, rows), check_vma=False
    )
```
